256 devices in a mesh: row: 8 (over y, x_lo), col: 32 (over z, x_hi, core).
Axes of the slice: x: 4 (x_hi: 2, x_lo: 2; x = x_hi * 2 + x_lo), y: 4, z: 8, core: 2. Of those that a mesh axis runs over, the one named last changes fastest.
Arguments:
- pair_rep: bfloat16 [1024, 1024, 128], P('row', 'col'), may hold values from -6 to 6
- proj_weight: bfloat16 [2, 4, 128, 128], replicated, may hold values from -0.5 to 0.5
- gate_weight: bfloat16 [2, 128, 128], replicated, may hold values from -0.5 to 0.5
- out_weight: bfloat16 [2, 128, 128], replicated, may hold values from -0.5 to 0.5
- in_gain: float32 [2, 128], replicated, may hold values from 0.1 to 1.9
- out_gain: float32 [2, 128], replicated, may hold values from 0.1 to 1.9
Outputs:
- updated_pair: bfloat16 [1024, 1024, 128], P('row', 'col')
The draws below stay inside these ranges and needn't reach their ends.
All inputs are finite; a program needn't handle non-finite values.
Results may differ from the reference program's by a relative error of at most 0.011.
Values may be sent and summed in bfloat16 or wider, within the bound.
No kernel may reach another device: no remote copies, remote signals or barrier semaphores. Data moves between devices by JAX's collectives and lax.ppermute only.
A program may use at most 64 MiB of HBM per device.

```python
import math
import jax
import jax.numpy as jnp
from jax import lax

C = 128
H = 128
N = 1024


def steps_of(own_key, extent, cuts, smallest, largest):
    def one(position, parts):
        draws = jax.random.uniform(jax.random.fold_in(jax.random.fold_in(own_key, 6), position), (parts,), jnp.float32, smallest / len(cuts), largest / len(cuts))
        return jnp.repeat(jnp.exp(draws), extent[position] // parts).reshape((-1,) + (1,) * (len(extent) - position - 1))

    level = one(*cuts[0])
    for cut in cuts[1:]:
        level = level * one(*cut)
    return level


def noise(key, extent, deviation, most, cuts=(), kind=jnp.bfloat16):
    entries = jax.random.normal(key, extent, jnp.float32) * deviation
    if len(cuts) > 0:
        entries = steps_of(key, extent, cuts, -0.22, 0.18) * entries
    return jnp.clip(entries, min=-most, max=most).astype(kind)


def setup_inputs(seed: int = 0) -> dict:
    arg_keys = jax.random.split(jax.random.key(seed), 7)
    pair_rep = noise(arg_keys[0], (N, N, C), 1.0, 6.0, ((0, 8), (1, 32)))
    proj_weight = noise(arg_keys[1], (2, 4, C, H), C ** -0.5, 0.5)
    gate_weight = noise(arg_keys[2], (2, C, C), C ** -0.5, 0.5)
    out_weight = noise(arg_keys[3], (2, H, C), H ** -0.5, 0.5)
    in_gain = jnp.clip(1.0 + 0.18 * jax.random.normal(arg_keys[4], (2, C), jnp.float32), 0.1, 1.9)
    out_gain = jnp.clip(1.0 + 0.18 * jax.random.normal(arg_keys[5], (2, H), jnp.float32), 0.1, 1.9)
    return dict(pair_rep=pair_rep, proj_weight=proj_weight, gate_weight=gate_weight, out_weight=out_weight, in_gain=in_gain, out_gain=out_gain)


epsilon = 1e-05

def layer_norm(values, gain_row):
    center = values - lax.optimization_barrier(jnp.mean(values, axis=-1, keepdims=True))
    spread = lax.optimization_barrier(jnp.mean(center * center, axis=-1, keepdims=True))
    return center * lax.rsqrt(spread + epsilon) * gain_row

def reference(pair_rep, proj_weight, gate_weight, out_weight, in_gain, out_gain):
    row_block = math.gcd(N, 64)
    channel_block = math.gcd(H, 16)
    current = pair_rep
    for update_index in range(2):
        weight_joined = jnp.transpose(proj_weight[update_index], (1, 0, 2)).reshape(C, 4 * H)

        def project(row_slab):
            widened = row_slab.astype(jnp.float32)
            normed = layer_norm(widened, in_gain[update_index]).astype(jnp.bfloat16)
            projected = jnp.dot(normed, weight_joined, preferred_element_type=jnp.float32)
            left_hand = (jax.nn.sigmoid(projected[..., 0:H]) * projected[..., H:2 * H]).astype(jnp.bfloat16)
            right_hand = (jax.nn.sigmoid(projected[..., 2 * H:3 * H]) * projected[..., 3 * H:4 * H]).astype(jnp.bfloat16)
            gating = jax.nn.sigmoid(jnp.dot(normed, gate_weight[update_index], preferred_element_type=jnp.float32))
            return (left_hand, right_hand, gating)
        blocks = current.reshape(N // row_block, row_block, N, C)
        left_hand, right_hand, gating = lax.map(project, blocks)
        left_channels = jnp.moveaxis(left_hand.reshape(N, N, H), 2, 0).reshape(H // channel_block, channel_block, N, N)
        right_channels = jnp.moveaxis(right_hand.reshape(N, N, H), 2, 0).reshape(H // channel_block, channel_block, N, N)
        pattern = 'hik,hjk->hij' if update_index == 0 else 'hki,hkj->hij'

        def contract(operands):
            return jnp.einsum(pattern, operands[0].astype(jnp.float32), operands[1].astype(jnp.float32)).astype(jnp.bfloat16)
        triangle = lax.map(contract, (left_channels, right_channels))
        triangle = jnp.moveaxis(triangle.reshape(H, N, N), 0, 2)

        def finish(pieces):
            triangle_rows, gate_rows, old_rows = pieces
            mixed = layer_norm(triangle_rows.astype(jnp.float32), out_gain[update_index]).astype(jnp.bfloat16)
            update = jnp.dot(mixed, out_weight[update_index], preferred_element_type=jnp.float32)
            return (old_rows.astype(jnp.float32) + gate_rows * update).astype(jnp.bfloat16)
        current = lax.map(finish, (triangle.reshape(N // row_block, row_block, N, H), gating, blocks)).reshape(N, N, C)
    return current
```

```python
import jax
import jax.numpy as jnp
from jax import lax
from jax.sharding import Mesh
from jax.sharding import PartitionSpec as P

CHIPS = ("row", "half")
SWAP = [(0, 1), (1, 0)]


epsilon = 1e-05


def layer_norm(values, gain_row, reduce_axis):
    center = values - jnp.mean(values, axis=reduce_axis, keepdims=True)
    spread = jnp.mean(center * center, axis=reduce_axis, keepdims=True)
    return center * lax.rsqrt(spread + epsilon) * gain_row


def to_chips(pieces):
    return lax.all_to_all(pieces, CHIPS, split_axis=0, concat_axis=0, tiled=True)


def local(pair_rep, proj_weight, gate_weight, out_weight, in_gain, out_gain):
    core = lax.axis_index("core")
    current = pair_rep
    for update_index in range(2):
        widened = current.astype(jnp.float32)
        normed = layer_norm(widened, in_gain[update_index], 2).astype(jnp.bfloat16)
        projected = jnp.einsum(
            "ijc,pch->phji", normed, proj_weight[update_index], preferred_element_type=jnp.float32
        )
        left_hand = (jax.nn.sigmoid(projected[0]) * projected[1]).astype(jnp.bfloat16)
        right_hand = (jax.nn.sigmoid(projected[2]) * projected[3]).astype(jnp.bfloat16)
        gating = jax.nn.sigmoid(
            jnp.dot(normed, gate_weight[update_index], preferred_element_type=jnp.float32)
        )
        operands = to_chips(jnp.stack([left_hand, right_hand], axis=1)).reshape(8, 16, 2, 32, 128)
        left, right = operands[:, :, 0], operands[:, :, 1]
        if update_index == 0:
            product = jnp.einsum(
                "rqsf,tqsg->rtgf", left, right, preferred_element_type=jnp.float32
            ).reshape(8, 16, 2, 32, 128)
            kept = lax.dynamic_index_in_dim(product, core, 2, keepdims=False)
            given = lax.dynamic_index_in_dim(product, 1 - core, 2, keepdims=False)
            taken = lax.ppermute(given.astype(jnp.bfloat16), "core", SWAP)
            triangle = (kept + taken.astype(jnp.float32)).astype(jnp.bfloat16)
        else:
            other = lax.ppermute(left, "core", SWAP)
            first = core == 0
            whole = jnp.stack(
                [jnp.where(first, left, other), jnp.where(first, other, left)], axis=2
            ).reshape(8, 8, 128, 128)
            triangle = jnp.einsum(
                "rbif,rqsf->bqsi", whole, right, preferred_element_type=jnp.float32
            ).astype(jnp.bfloat16)
        returned = to_chips(triangle.reshape(128, 32, 128))
        mixed = layer_norm(
            returned.astype(jnp.float32), out_gain[update_index][:, None, None], 0
        ).astype(jnp.bfloat16)
        update = jnp.einsum(
            "hji,hc->ijc", mixed, out_weight[update_index], preferred_element_type=jnp.float32
        )
        current = (widened + gating * update).astype(jnp.bfloat16)
    return current


def solution(mesh):
    finer = Mesh(mesh.devices.reshape(8, 16, 2), ("row", "half", "core"))
    placed = (P("row", ("half", "core"), None), P(), P(), P(), P(), P())
    return jax.shard_map(
        local, mesh=finer, in_specs=placed, out_specs=P("row", ("half", "core"), None), check_vma=False
    )
```

```python
import jax
import jax.numpy as jnp
from jax import lax
from jax.experimental import pallas as pl
from jax.experimental.pallas import tpu as pltpu
from jax.sharding import Mesh
from jax.sharding import PartitionSpec as P

CHIPS = ("row", "half")
SWAP = [(0, 1), (1, 0)]
F32 = jnp.float32
BF16 = jnp.bfloat16
PITCH = 40
WIDE = 136


epsilon = 1e-05


def dot(a, b):
    return lax.dot_general(a, b, (((1,), (0,)), ((), ())), preferred_element_type=F32)


def sigmoid(values):
    return 0.5 * jnp.tanh(0.5 * values) + 0.5


def layer_norm(values, gain):
    center = values - jnp.sum(values, axis=0, keepdims=True) * (1.0 / 128)
    spread = jnp.sum(center * center, axis=0, keepdims=True) * (1.0 / 128)
    return center * lax.rsqrt(spread + epsilon) * gain


def column(row):
    return jnp.broadcast_to(row, (128, 128)).T


def turn(matrix):
    return matrix.astype(F32).T.astype(BF16)


def spread_rows(source, scratch):
    def step(n, _):
        for part in range(4):
            at = n * 4 + part
            scratch[pl.ds(pl.multiple_of(at * PITCH, 8), 32), :] = source[at].astype(F32)
        return _

    lax.fori_loop(0, 32, step, 0)


def project(channels, gain, weights, hands, j):
    normed = layer_norm(channels, gain).astype(BF16)
    projected = dot(weights[...], normed)
    at = pl.ds(pl.multiple_of(j * WIDE, 8), 128)
    hands[0, at, :] = sigmoid(projected[0:128]) * projected[128:256]
    hands[1, at, :] = sigmoid(projected[256:384]) * projected[384:512]


def gather_hands(hands, send):
    def step(n, _):
        for part in range(4):
            h = n * 4 + part
            for side in range(2):
                send[h, side] = hands[side, pl.ds(h, 32, stride=WIDE), :].astype(BF16)
        return _

    lax.fori_loop(0, 32, step, 0)


def set_weights(weights, proj, update_index):
    for p in range(4):
        weights[p * 128 : (p + 1) * 128, :] = turn(proj[update_index, p])


def first_kernel(x, proj, in_gain, send, turned, rows, hands, weights):
    set_weights(weights, proj, 0)
    gain = column(in_gain[0:1, :])
    spread_rows(x, rows)

    def step(j, _):
        channels = rows[pl.ds(j, 128, stride=PITCH), :].T
        turned[j] = channels.astype(BF16)
        project(channels, gain, weights, hands, j)
        return _

    lax.fori_loop(0, 32, step, 0, unroll=2)
    gather_hands(hands, send)


def new_channels(update_index, tri, turned, gain_in, gain_out, gate, out, j):
    mixed = layer_norm(tri[pl.ds(j, 128, stride=PITCH), :], gain_out).astype(BF16)
    change = dot(out, mixed)
    old = turned[j].astype(F32)
    normed = layer_norm(old, gain_in).astype(BF16)
    return old + sigmoid(dot(gate, normed)) * change


def middle_kernel(returned, turned, proj, gate_w, out_w, in_gain, out_gain, send, newer, tri, hands, weights):
    set_weights(weights, proj, 1)
    gain_in, gain_out, gain_next = column(in_gain[0:1, :]), column(out_gain[0:1, :]), column(in_gain[1:2, :])
    gate, out = turn(gate_w[0]), turn(out_w[0])
    spread_rows(returned, tri)

    def step(j, _):
        channels = new_channels(0, tri, turned, gain_in, gain_out, gate, out, j).astype(BF16)
        newer[j] = channels
        project(channels.astype(F32), gain_next, weights, hands, j)
        return _

    lax.fori_loop(0, 32, step, 0, unroll=2)
    gather_hands(hands, send)


def last_kernel(returned, turned, gate_w, out_w, in_gain, out_gain, final, tri, rows):
    gain_in, gain_out = column(in_gain[1:2, :]), column(out_gain[1:2, :])
    gate, out = turn(gate_w[1]), turn(out_w[1])
    spread_rows(returned, tri)

    def step(j, _):
        channels = new_channels(1, tri, turned, gain_in, gain_out, gate, out, j)
        rows[pl.ds(j, 128, stride=PITCH), :] = channels.T
        return _

    lax.fori_loop(0, 32, step, 0, unroll=2)

    def collect(n, _):
        for part in range(4):
            at = n * 4 + part
            final[at] = rows[pl.ds(pl.multiple_of(at * PITCH, 8), 32), :].astype(BF16)
        return _

    lax.fori_loop(0, 32, collect, 0)


def side_of(operands, r, side):
    return operands[r, :, side].reshape(512, 128)


def given_kernel(core, operands, given, kept_rows, lefts, turned):
    for r in range(8):
        lefts[:, r * 128 : (r + 1) * 128] = side_of(operands, r, 0)
        turned[r * 128 : (r + 1) * 128, :] = turn(side_of(operands, r, 1))
    for q in range(16):
        kept_rows[q * 32 : (q + 1) * 32, :] = turned[
            pl.ds(pl.multiple_of(q * 64 + core[0] * 32, 32), 32), :
        ]
    for q in range(0, 16, 4):
        block = jnp.concatenate(
            [turned[pl.ds(pl.multiple_of(p * 64 + 32 - core[0] * 32, 32), 32), :] for p in range(q, q + 4)], axis=0
        )
        product = dot(block, lefts[...]).astype(BF16)
        for r in range(8):
            given[r, q : q + 4] = product[:, r * 128 : (r + 1) * 128].reshape(4, 32, 128)


def kept_kernel(kept_rows, operands, kept):
    lefts = jnp.concatenate([side_of(operands, r, 0) for r in range(8)], axis=1)
    for q in range(0, 16, 4):
        product = dot(kept_rows[q * 32 : (q + 4) * 32, :], lefts)
        for r in range(8):
            kept[r, q : q + 4] = product[:, r * 128 : (r + 1) * 128].reshape(4, 32, 128)


def incoming_kernel(core, operands, other, products, lefts):
    for r in range(8):
        for q in range(16):
            own = pl.multiple_of(q * 64 + core[0] * 32, 32)
            swapped = pl.multiple_of(q * 64 + 32 - core[0] * 32, 32)
            lefts[pl.ds(own, 32), r * 128 : (r + 1) * 128] = operands[r, q, 0]
            lefts[pl.ds(swapped, 32), r * 128 : (r + 1) * 128] = other[r, q]
    rights = jnp.concatenate([side_of(operands, r, 1) for r in range(8)], axis=1)
    for b in range(0, 8, 2):
        product = lax.dot_general(
            rights, lefts[b * 128 : (b + 2) * 128, :], (((1,), (1,)), ((), ())), preferred_element_type=F32
        ).astype(BF16)
        for part in range(2):
            products[b + part] = product[:, part * 128 : (part + 1) * 128].reshape(16, 32, 128)


def shape(dims, kind=BF16):
    return jax.ShapeDtypeStruct(dims, kind)


def call(body, outs, scratch, *args, scalars=0):
    vmem = pl.BlockSpec(memory_space=pltpu.VMEM)
    smem = pl.BlockSpec(memory_space=pltpu.SMEM)
    return pl.pallas_call(
        body,
        out_shape=outs,
        in_specs=[smem] * scalars + [vmem] * (len(args) - scalars),
        out_specs=[vmem] * len(outs),
        scratch_shapes=[pltpu.VMEM(dims, kind) for dims, kind in scratch],
        compiler_params=pltpu.CompilerParams(vmem_limit_bytes=48 * 1024 * 1024),
        name=body.__name__,
    )(*args)


def to_chips(pieces):
    return lax.all_to_all(pieces, CHIPS, split_axis=0, concat_axis=0, tiled=True)


ROWS = ((128 * PITCH, 128), F32)
HANDS = ((2, 32 * WIDE, 128), F32)
WEIGHTS = ((512, 128), BF16)
SEND = shape((128, 2, 32, 128))
TURNED = shape((32, 128, 128))
HALF = (8, 16, 32, 128)


def local(pair_rep, proj_weight, gate_weight, out_weight, in_gain, out_gain):
    core = lax.axis_index("core").astype(jnp.int32).reshape(1)
    send, turned = call(first_kernel, [SEND, TURNED], [ROWS, HANDS, WEIGHTS], pair_rep, proj_weight, in_gain)
    operands = to_chips(send).reshape(8, 16, 2, 32, 128)
    given, kept_rows = call(
        given_kernel,
        [shape(HALF), shape((512, 512))],
        [((512, 1024), BF16), ((1024, 512), BF16)],
        core,
        operands,
        scalars=1,
    )
    taken = lax.ppermute(given, "core", SWAP)
    (kept,) = call(kept_kernel, [shape(HALF, F32)], [], kept_rows, operands)
    triangle = (kept + taken.astype(F32)).astype(BF16)
    returned = to_chips(triangle.reshape(128, 32, 128))
    send, turned = call(
        middle_kernel,
        [SEND, TURNED],
        [ROWS, HANDS, WEIGHTS],
        returned,
        turned,
        proj_weight,
        gate_weight,
        out_weight,
        in_gain,
        out_gain,
    )
    operands = to_chips(send).reshape(8, 16, 2, 32, 128)
    other = lax.ppermute(operands[:, :, 0], "core", SWAP)
    (triangle,) = call(incoming_kernel, [shape(HALF)], [((1024, 1024), BF16)], core, operands, other, scalars=1)
    returned = to_chips(triangle.reshape(128, 32, 128))
    (final,) = call(
        last_kernel,
        [shape((128, 32, 128))],
        [ROWS, ROWS],
        returned,
        turned,
        gate_weight,
        out_weight,
        in_gain,
        out_gain,
    )
    return final


def solution(mesh):
    finer = Mesh(mesh.devices.reshape(8, 16, 2), ("row", "half", "core"))
    placed = (P("row", ("half", "core"), None), P(), P(), P(), P(), P())
    return jax.shard_map(
        local, mesh=finer, in_specs=placed, out_specs=P("row", ("half", "core"), None), check_vma=False
    )
```

```python
import jax
import jax.numpy as jnp
from jax import lax
from jax.experimental import pallas as pl
from jax.experimental.pallas import tpu as pltpu
from jax.sharding import Mesh
from jax.sharding import PartitionSpec as P

CHIPS = ("row", "half")
SWAP = [(0, 1), (1, 0)]
F32 = jnp.float32
BF16 = jnp.bfloat16
PITCH = 40
WIDE = 136


epsilon = 1e-05


def dot(a, b):
    return lax.dot_general(a, b, (((1,), (0,)), ((), ())), preferred_element_type=F32)


def sigmoid(values):
    return 0.5 * jnp.tanh(0.5 * values) + 0.5


def layer_norm(values, gain):
    center = values - jnp.sum(values, axis=0, keepdims=True) * (1.0 / 128)
    spread = jnp.sum(center * center, axis=0, keepdims=True) * (1.0 / 128)
    return center * lax.rsqrt(spread + epsilon) * gain


def column(row):
    return jnp.broadcast_to(row, (128, 128)).T


def turn(matrix):
    return matrix.astype(F32).T.astype(BF16)


def spread_rows(source, scratch):
    def step(n, _):
        for part in range(8):
            at = n * 8 + part
            scratch[pl.ds(pl.multiple_of(at * PITCH, 8), 32), :] = source[at].astype(F32)
        return _

    lax.fori_loop(0, 16, step, 0)


def each(steps, body):
    def step(j, _):
        body(j)
        return _

    lax.fori_loop(0, steps, step, 0, unroll=8)


def side_by_side(blocks, pair):
    return jnp.concatenate([blocks[pair * 2], blocks[pair * 2 + 1]], axis=1)


def project(normed, weights, hands):
    def body(pair):
        both = side_by_side(normed, pair)
        for side in range(2):
            projected = dot(weights[side * 256 : (side + 1) * 256, :], both)
            hand = sigmoid(projected[0:128]) * projected[128:256]
            for part in range(2):
                at = pl.ds(pl.multiple_of((pair * 2 + part) * WIDE, 8), 128)
                hands[side, at, :] = hand[:, part * 128 : (part + 1) * 128]

    each(16, body)


def gather_hands(hands, send):
    def step(n, _):
        for part in range(8):
            h = n * 8 + part
            for side in range(2):
                send[h, side] = hands[side, pl.ds(h, 32, stride=WIDE), :].astype(BF16)
        return _

    lax.fori_loop(0, 16, step, 0)


def set_weights(weights, proj, update_index):
    for p in range(4):
        weights[p * 128 : (p + 1) * 128, :] = turn(proj[update_index, p])


def first_kernel(x, proj, in_gain, send, turned, rows, hands, normed, weights, gains):
    set_weights(weights, proj, 0)
    gains[0] = column(in_gain[0:1, :])
    spread_rows(x, rows)

    def body(j):
        channels = rows[pl.ds(j, 128, stride=PITCH), :].T
        turned[j] = channels.astype(BF16)
        normed[j] = layer_norm(channels, gains[0]).astype(BF16)

    each(32, body)
    project(normed, weights, hands)
    gather_hands(hands, send)


def norm_both(tri, turned, mixed, normed, gains):
    def body(j):
        mixed[j] = layer_norm(tri[pl.ds(j, 128, stride=PITCH), :], gains[1]).astype(BF16)
        normed[j] = layer_norm(turned[j].astype(F32), gains[0]).astype(BF16)

    each(32, body)


def new_channels(turned, mixed, normed, gate, out, pair):
    change = dot(out[...], side_by_side(mixed, pair))
    gating = sigmoid(dot(gate[...], side_by_side(normed, pair)))
    added = gating * change
    return [
        turned[pair * 2 + part].astype(F32) + added[:, part * 128 : (part + 1) * 128]
        for part in range(2)
    ]


def middle_kernel(
    returned, turned, proj, gate_w, out_w, in_gain, out_gain, send, newer,
    tri, hands, mixed, normed, later, weights, gate, out, gains,
):
    set_weights(weights, proj, 1)
    gate[...], out[...] = turn(gate_w[0]), turn(out_w[0])
    gains[0], gains[1], gains[2] = column(in_gain[0:1, :]), column(out_gain[0:1, :]), column(in_gain[1:2, :])
    spread_rows(returned, tri)
    norm_both(tri, turned, mixed, normed, gains)

    def body(pair):
        for part, channels in enumerate(new_channels(turned, mixed, normed, gate, out, pair)):
            rounded = channels.astype(BF16)
            newer[pair * 2 + part] = rounded
            later[pair * 2 + part] = layer_norm(rounded.astype(F32), gains[2]).astype(BF16)

    each(16, body)
    project(later, weights, hands)
    gather_hands(hands, send)


def last_kernel(returned, turned, gate_w, out_w, in_gain, out_gain, final, tri, rows, mixed, normed, newer, gate, out, gains):
    gate[...], out[...] = turn(gate_w[1]), turn(out_w[1])
    gains[0], gains[1] = column(in_gain[1:2, :]), column(out_gain[1:2, :])
    spread_rows(returned, tri)
    norm_both(tri, turned, mixed, normed, gains)

    def body(pair):
        for part, channels in enumerate(new_channels(turned, mixed, normed, gate, out, pair)):
            newer[pair * 2 + part] = channels

    each(16, body)

    def back(j):
        rows[pl.ds(j, 128, stride=PITCH), :] = newer[j].T

    each(32, back)

    def collect(n, _):
        for part in range(8):
            at = n * 8 + part
            final[at] = rows[pl.ds(pl.multiple_of(at * PITCH, 8), 32), :].astype(BF16)
        return _

    lax.fori_loop(0, 16, collect, 0)


def side_of(operands, r, side):
    return operands[r, :, side].reshape(512, 128)


def given_kernel(core, operands, given, kept_rows, lefts, turned):
    for r in range(8):
        lefts[:, r * 128 : (r + 1) * 128] = side_of(operands, r, 0)
        turned[r * 128 : (r + 1) * 128, :] = turn(side_of(operands, r, 1))
    for q in range(16):
        kept_rows[q * 32 : (q + 1) * 32, :] = turned[
            pl.ds(pl.multiple_of(q * 64 + core[0] * 32, 32), 32), :
        ]
    for q in range(0, 16, 4):
        block = jnp.concatenate(
            [turned[pl.ds(pl.multiple_of(p * 64 + 32 - core[0] * 32, 32), 32), :] for p in range(q, q + 4)], axis=0
        )
        product = dot(block, lefts[...]).astype(BF16)
        for r in range(8):
            given[r, q : q + 4] = product[:, r * 128 : (r + 1) * 128].reshape(4, 32, 128)


def kept_kernel(kept_rows, operands, kept):
    lefts = jnp.concatenate([side_of(operands, r, 0) for r in range(8)], axis=1)
    for q in range(0, 16, 4):
        product = dot(kept_rows[q * 32 : (q + 4) * 32, :], lefts)
        for r in range(8):
            kept[r, q : q + 4] = product[:, r * 128 : (r + 1) * 128].reshape(4, 32, 128)


def incoming_kernel(core, operands, other, products, lefts):
    for r in range(8):
        for q in range(16):
            own = pl.multiple_of(q * 64 + core[0] * 32, 32)
            swapped = pl.multiple_of(q * 64 + 32 - core[0] * 32, 32)
            lefts[pl.ds(own, 32), r * 128 : (r + 1) * 128] = operands[r, q, 0]
            lefts[pl.ds(swapped, 32), r * 128 : (r + 1) * 128] = other[r, q]
    rights = jnp.concatenate([side_of(operands, r, 1) for r in range(8)], axis=1)
    for b in range(0, 8, 2):
        product = lax.dot_general(
            rights, lefts[b * 128 : (b + 2) * 128, :], (((1,), (1,)), ((), ())), preferred_element_type=F32
        ).astype(BF16)
        for part in range(2):
            products[b + part] = product[:, part * 128 : (part + 1) * 128].reshape(16, 32, 128)


def shape(dims, kind=BF16):
    return jax.ShapeDtypeStruct(dims, kind)


def call(body, outs, scratch, *args, scalars=0):
    vmem = pl.BlockSpec(memory_space=pltpu.VMEM)
    smem = pl.BlockSpec(memory_space=pltpu.SMEM)
    return pl.pallas_call(
        body,
        out_shape=outs,
        in_specs=[smem] * scalars + [vmem] * (len(args) - scalars),
        out_specs=[vmem] * len(outs),
        scratch_shapes=[pltpu.VMEM(dims, kind) for dims, kind in scratch],
        compiler_params=pltpu.CompilerParams(vmem_limit_bytes=48 * 1024 * 1024),
        name=body.__name__,
    )(*args)


def to_chips(pieces):
    return lax.all_to_all(pieces, CHIPS, split_axis=0, concat_axis=0, tiled=True)


ROWS = ((128 * PITCH, 128), F32)
BLOCKS = ((32, 128, 128), BF16)
SQUARE = ((128, 128), BF16)
GAINS = ((3, 128, 128), F32)
HANDS = ((2, 32 * WIDE, 128), F32)
WEIGHTS = ((512, 128), BF16)
SEND = shape((128, 2, 32, 128))
TURNED = shape((32, 128, 128))
HALF = (8, 16, 32, 128)


def local(pair_rep, proj_weight, gate_weight, out_weight, in_gain, out_gain):
    core = lax.axis_index("core").astype(jnp.int32).reshape(1)
    core, pair_rep = lax.optimization_barrier((core, pair_rep))
    send, turned = call(first_kernel, [SEND, TURNED], [ROWS, HANDS, BLOCKS, WEIGHTS, GAINS], pair_rep, proj_weight, in_gain)
    operands = to_chips(send).reshape(8, 16, 2, 32, 128)
    given, kept_rows = call(
        given_kernel,
        [shape(HALF), shape((512, 512))],
        [((512, 1024), BF16), ((1024, 512), BF16)],
        core,
        operands,
        scalars=1,
    )
    taken = lax.ppermute(given, "core", SWAP)
    (kept,) = call(kept_kernel, [shape(HALF, F32)], [], kept_rows, operands)
    triangle = (kept + taken.astype(F32)).astype(BF16)
    returned = to_chips(triangle.reshape(128, 32, 128))
    send, turned = call(
        middle_kernel,
        [SEND, TURNED],
        [ROWS, HANDS, BLOCKS, BLOCKS, BLOCKS, WEIGHTS, SQUARE, SQUARE, GAINS],
        returned,
        turned,
        proj_weight,
        gate_weight,
        out_weight,
        in_gain,
        out_gain,
    )
    operands = to_chips(send).reshape(8, 16, 2, 32, 128)
    other = lax.ppermute(operands[:, :, 0], "core", SWAP)
    (triangle,) = call(incoming_kernel, [shape(HALF)], [((1024, 1024), BF16)], core, operands, other, scalars=1)
    returned = to_chips(triangle.reshape(128, 32, 128))
    (final,) = call(
        last_kernel,
        [shape((128, 32, 128))],
        [ROWS, ROWS, BLOCKS, BLOCKS, ((32, 128, 128), F32), SQUARE, SQUARE, GAINS],
        returned,
        turned,
        gate_weight,
        out_weight,
        in_gain,
        out_gain,
    )
    return final


def solution(mesh):
    finer = Mesh(mesh.devices.reshape(8, 16, 2), ("row", "half", "core"))
    placed = (P("row", ("half", "core"), None), P(), P(), P(), P(), P())
    return jax.shard_map(
        local, mesh=finer, in_specs=placed, out_specs=P("row", ("half", "core"), None), check_vma=False
    )
```

```python
import functools

import jax
import jax.numpy as jnp
from jax import lax
from jax.experimental import pallas as pl
from jax.experimental.pallas import tpu as pltpu
from jax.sharding import Mesh
from jax.sharding import PartitionSpec as P

CHIPS = ("row", "half")
SWAP = [(0, 1), (1, 0)]
F32 = jnp.float32
BF16 = jnp.bfloat16
PITCH = 40
WIDE = 136


epsilon = 1e-05


def dot(a, b):
    return lax.dot_general(a, b, (((1,), (0,)), ((), ())), preferred_element_type=F32)


def sigmoid(values):
    return 0.5 * jnp.tanh(0.5 * values) + 0.5


def layer_norm(values, gain):
    center = values - jnp.sum(values, axis=0, keepdims=True) * (1.0 / 128)
    spread = jnp.sum(center * center, axis=0, keepdims=True) * (1.0 / 128)
    return center * lax.rsqrt(spread + epsilon) * gain


def column(row):
    return jnp.broadcast_to(row, (128, 128)).T


def turn(matrix):
    return matrix.astype(F32).T.astype(BF16)


def spread_rows(source, scratch, start, groups):
    def step(n, _):
        for part in range(8):
            at = start + n * 8 + part
            scratch[pl.ds(pl.multiple_of(at * PITCH, 8), 32), :] = source[at].astype(F32)
        return _

    lax.fori_loop(0, groups // 8, step, 0)


def each(steps, body):
    def step(j, _):
        body(j)
        return _

    lax.fori_loop(0, steps, step, 0, unroll=8)


def side_by_side(blocks, pair):
    return jnp.concatenate([blocks[pair * 2], blocks[pair * 2 + 1]], axis=1)


def project(normed, weights, hands):
    def body(pair):
        both = side_by_side(normed, pair)
        for side in range(2):
            projected = dot(weights[side * 256 : (side + 1) * 256, :], both)
            hand = sigmoid(projected[0:128]) * projected[128:256]
            for part in range(2):
                at = pl.ds(pl.multiple_of((pair * 2 + part) * WIDE, 8), 128)
                hands[side, at, :] = hand[:, part * 128 : (part + 1) * 128]

    each(16, body)


def gather_hands(hands, send):
    def step(n, _):
        for part in range(8):
            h = n * 8 + part
            for side in range(2):
                send[h, side] = hands[side, pl.ds(h, 32, stride=WIDE), :].astype(BF16)
        return _

    lax.fori_loop(0, 16, step, 0)


def fetch(pairs, arrived):
    copies = [pltpu.make_async_copy(far, near, arrived.at[n]) for n, (far, near) in enumerate(pairs)]
    for copy in copies:
        copy.start()
    return copies


def first_kernel(x, proj, in_gain, send, turned, x_near, proj_near, gain_near, rows, hands, normed, weights, gains, arrived):
    quarters = [pl.ds(n * 32, 32) for n in range(4)]
    pairs = [(x.at[part], x_near.at[part]) for part in quarters]
    pieces = fetch([*pairs, (proj.at[0], proj_near), (in_gain, gain_near)], arrived)
    for n in range(4):
        pieces[n].wait()
        spread_rows(x_near, rows, n * 32, 32)
    pieces[4].wait()
    pieces[5].wait()
    for p in range(4):
        weights[p * 128 : (p + 1) * 128, :] = turn(proj_near[p])
    gains[...] = column(gain_near[0:1, :])

    def body(j):
        channels = rows[pl.ds(j, 128, stride=PITCH), :].T
        turned[j] = channels.astype(BF16)
        normed[j] = layer_norm(channels, gains[...]).astype(BF16)

    each(32, body)
    project(normed, weights, hands)
    gather_hands(hands, send)


def side_kernel(update_index, turned, proj, gate_w, out_w, in_gain, out_gain, gating, out, gains, weights, normed, gate):
    gate[...], out[...] = turn(gate_w[update_index]), turn(out_w[update_index])
    gains[0] = column(out_gain[update_index : update_index + 1, :])
    gains[1] = column(in_gain[1:2, :])
    gains[2] = column(in_gain[update_index : update_index + 1, :])
    for p in range(4):
        weights[p * 128 : (p + 1) * 128, :] = turn(proj[1, p])

    def norm(j):
        normed[j] = layer_norm(turned[j].astype(F32), gains[2]).astype(BF16)

    each(32, norm)

    def body(pair):
        both = sigmoid(dot(gate[...], side_by_side(normed, pair)))
        for part in range(2):
            gating[pair * 2 + part] = both[:, part * 128 : (part + 1) * 128]

    each(16, body)


def mix(tri, mixed, gains):
    def body(j):
        mixed[j] = layer_norm(tri[pl.ds(j, 128, stride=PITCH), :], gains[0]).astype(BF16)

    each(32, body)


def new_channels(turned, gating, mixed, out, pair):
    change = dot(out[...], side_by_side(mixed, pair))
    return [
        turned[pair * 2 + part].astype(F32) + gating[pair * 2 + part] * change[:, part * 128 : (part + 1) * 128]
        for part in range(2)
    ]


def middle_kernel(
    far_gains, far_out, far_gating, far_turned, far_weights, returned, send, newer,
    gains, out, gating, turned, weights, tri, hands, mixed, later, arrived,
):
    pieces = fetch(
        [(far_gains, gains), (far_out, out), (far_gating, gating), (far_turned, turned), (far_weights, weights)],
        arrived,
    )
    spread_rows(returned, tri, 0, 128)
    pieces[0].wait()
    mix(tri, mixed, gains)
    for piece in pieces[1:]:
        piece.wait()

    def body(pair):
        for part, channels in enumerate(new_channels(turned, gating, mixed, out, pair)):
            rounded = channels.astype(BF16)
            newer[pair * 2 + part] = rounded
            later[pair * 2 + part] = layer_norm(rounded.astype(F32), gains[1]).astype(BF16)

    each(16, body)
    project(later, weights, hands)
    gather_hands(hands, send)


def last_kernel(
    far_gains, far_out, far_gating, far_turned, returned, final,
    gains, out, gating, turned, tri, rows, mixed, newer, near, arrived, left,
):
    pieces = fetch([(far_gains, gains), (far_out, out), (far_gating, gating), (far_turned, turned)], arrived)
    spread_rows(returned, tri, 0, 128)
    pieces[0].wait()
    mix(tri, mixed, gains)
    for piece in pieces[1:]:
        piece.wait()

    def body(pair):
        for part, channels in enumerate(new_channels(turned, gating, mixed, out, pair)):
            newer[pair * 2 + part] = channels

    each(16, body)

    def back(j):
        rows[pl.ds(j, 128, stride=PITCH), :] = newer[j].T

    each(32, back)
    pieces = []
    for n in range(4):

        def collect(m, _):
            for part in range(8):
                at = n * 32 + m * 8 + part
                near[at] = rows[pl.ds(pl.multiple_of(at * PITCH, 8), 32), :].astype(BF16)
            return _

        lax.fori_loop(0, 4, collect, 0)
        pieces.append(pltpu.make_async_copy(near.at[pl.ds(n * 32, 32)], final.at[pl.ds(n * 32, 32)], left.at[n]))
        pieces[n].start()
    for piece in pieces:
        piece.wait()


def side_of(operands, r, side):
    return operands[r, :, side].reshape(512, 128)


def given_kernel(core, operands, given, kept_rows, lefts, turned):
    for r in range(8):
        lefts[:, r * 128 : (r + 1) * 128] = side_of(operands, r, 0)
        turned[r * 128 : (r + 1) * 128, :] = turn(side_of(operands, r, 1))
    for q in range(16):
        kept_rows[q * 32 : (q + 1) * 32, :] = turned[
            pl.ds(pl.multiple_of(q * 64 + core[0] * 32, 32), 32), :
        ]
    for q in range(0, 16, 4):
        block = jnp.concatenate(
            [turned[pl.ds(pl.multiple_of(p * 64 + 32 - core[0] * 32, 32), 32), :] for p in range(q, q + 4)], axis=0
        )
        product = dot(block, lefts[...]).astype(BF16)
        for r in range(8):
            given[r, q : q + 4] = product[:, r * 128 : (r + 1) * 128].reshape(4, 32, 128)


def kept_kernel(kept_rows, operands, kept):
    lefts = jnp.concatenate([side_of(operands, r, 0) for r in range(8)], axis=1)
    for q in range(0, 16, 4):
        product = dot(kept_rows[q * 32 : (q + 4) * 32, :], lefts)
        for r in range(8):
            kept[r, q : q + 4] = product[:, r * 128 : (r + 1) * 128].reshape(4, 32, 128)


def incoming_kernel(core, operands, other, products, lefts):
    for r in range(8):
        for q in range(16):
            own = pl.multiple_of(q * 64 + core[0] * 32, 32)
            swapped = pl.multiple_of(q * 64 + 32 - core[0] * 32, 32)
            lefts[pl.ds(own, 32), r * 128 : (r + 1) * 128] = operands[r, q, 0]
            lefts[pl.ds(swapped, 32), r * 128 : (r + 1) * 128] = other[r, q]
    rights = jnp.concatenate([side_of(operands, r, 1) for r in range(8)], axis=1)
    for b in range(0, 8, 2):
        product = lax.dot_general(
            rights, lefts[b * 128 : (b + 2) * 128, :], (((1,), (1,)), ((), ())), preferred_element_type=F32
        ).astype(BF16)
        for part in range(2):
            products[b + part] = product[:, part * 128 : (part + 1) * 128].reshape(16, 32, 128)


def shape(dims, kind=BF16):
    return jax.ShapeDtypeStruct(dims, kind)


def call(body, outs, scratch, *args, scalars=0, far=0, far_out=False, name=None):
    args = [
        pltpu.with_memory_space_constraint(arg, pltpu.HBM) if scalars <= n < scalars + far else arg
        for n, arg in enumerate(args)
    ]
    vmem, smem, hbm = (pl.BlockSpec(memory_space=space) for space in (pltpu.VMEM, pltpu.SMEM, pltpu.HBM))
    return pl.pallas_call(
        body,
        out_shape=outs,
        in_specs=[smem] * scalars + [hbm] * far + [vmem] * (len(args) - scalars - far),
        out_specs=[hbm if far_out else vmem] * len(outs),
        scratch_shapes=[
            dims if kind is None else pltpu.VMEM(dims, kind) for dims, kind in scratch
        ],
        compiler_params=pltpu.CompilerParams(vmem_limit_bytes=20 * 1024 * 1024),
        name=name or body.__name__,
    )(*args)


def to_chips(pieces):
    return lax.all_to_all(pieces, CHIPS, split_axis=0, concat_axis=0, tiled=True)


ROWS = ((128 * PITCH, 128), F32)
BLOCKS = ((32, 128, 128), BF16)
WHOLE = ((128, 32, 128), BF16)
SQUARE = ((128, 128), BF16)
GAINS = ((3, 128, 128), F32)
HANDS = ((2, 32 * WIDE, 128), F32)
WEIGHTS = ((512, 128), BF16)
SEND = shape((128, 2, 32, 128))
TURNED = shape(*BLOCKS)
HALF = (8, 16, 32, 128)


def first(pair_rep, proj_weight, in_gain):
    near = [WHOLE, ((4, 128, 128), BF16), ((2, 128), F32)]
    scratch = [*near, ROWS, HANDS, BLOCKS, WEIGHTS, ((128, 128), F32), (pltpu.SemaphoreType.DMA((6,)), None)]
    return call(first_kernel, [SEND, TURNED], scratch, pair_rep, proj_weight, in_gain, far=3)


def side(update_index, *args):
    outs = [shape(BLOCKS[0], F32), shape(*SQUARE), shape(*GAINS), shape(*WEIGHTS)]
    body = functools.partial(side_kernel, update_index)
    return call(body, outs, [BLOCKS, SQUARE], *args, name="side_kernel")


NEAR = [GAINS, SQUARE, (BLOCKS[0], F32), BLOCKS]


def copies(number):
    return (pltpu.SemaphoreType.DMA((number,)), None)


def middle(returned, turned, gating, out, gains, weights):
    scratch = [*NEAR, WEIGHTS, ROWS, HANDS, BLOCKS, BLOCKS, copies(5)]
    return call(middle_kernel, [SEND, TURNED], scratch, gains, out, gating, turned, weights, returned, far=5)


def last(returned, turned, gating, out, gains):
    scratch = [*NEAR, ROWS, ROWS, BLOCKS, (BLOCKS[0], F32), WHOLE, copies(4), copies(4)]
    return call(last_kernel, [shape(*WHOLE)], scratch, gains, out, gating, turned, returned, far=4, far_out=True)[0]


def local(pair_rep, proj_weight, gate_weight, out_weight, in_gain, out_gain):
    core = lax.axis_index("core").astype(jnp.int32).reshape(1)
    core, pair_rep = lax.optimization_barrier((core, pair_rep))
    parameters = (proj_weight, gate_weight, out_weight, in_gain, out_gain)
    send, turned = first(pair_rep, proj_weight, in_gain)
    operands = to_chips(send).reshape(8, 16, 2, 32, 128)
    gating, out, gains, weights = side(0, turned, *parameters)
    given, kept_rows = call(
        given_kernel,
        [shape(HALF), shape((512, 512))],
        [((512, 1024), BF16), ((1024, 512), BF16)],
        core,
        operands,
        scalars=1,
    )
    taken = lax.ppermute(given, "core", SWAP)
    (kept,) = call(kept_kernel, [shape(HALF, F32)], [], kept_rows, operands)
    triangle = (kept + taken.astype(F32)).astype(BF16)
    returned = to_chips(triangle.reshape(128, 32, 128))
    send, turned = middle(returned, turned, gating, out, gains, weights)
    operands = to_chips(send).reshape(8, 16, 2, 32, 128)
    gating, out, gains, _ = side(1, turned, *parameters)
    other = lax.ppermute(operands[:, :, 0], "core", SWAP)
    (triangle,) = call(incoming_kernel, [shape(HALF)], [((1024, 1024), BF16)], core, operands, other, scalars=1)
    returned = to_chips(triangle.reshape(128, 32, 128))
    return last(returned, turned, gating, out, gains)


def solution(mesh):
    finer = Mesh(mesh.devices.reshape(8, 16, 2), ("row", "half", "core"))
    placed = (P("row", ("half", "core"), None), P(), P(), P(), P(), P())
    return jax.shard_map(
        local, mesh=finer, in_specs=placed, out_specs=P("row", ("half", "core"), None), check_vma=False
    )
```

```python
import functools

import jax
import jax.numpy as jnp
from jax import lax
from jax.experimental import pallas as pl
from jax.experimental.pallas import tpu as pltpu
from jax.sharding import Mesh
from jax.sharding import PartitionSpec as P


CHIPS = ("row", "half")
SWAP = [(0, 1), (1, 0)]
F32 = jnp.float32
BF16 = jnp.bfloat16
PITCH = 40
WIDE = 136


epsilon = 1e-05


def dot(a, b):
    return lax.dot_general(a, b, (((1,), (0,)), ((), ())), preferred_element_type=F32)


def sigmoid(values):
    return 0.5 * jnp.tanh(0.5 * values) + 0.5


def layer_norm(values, gain):
    center = values - jnp.sum(values, axis=0, keepdims=True) * (1.0 / 128)
    spread = jnp.sum(center * center, axis=0, keepdims=True) * (1.0 / 128)
    return center * lax.rsqrt(spread + epsilon) * gain


def column(row):
    return jnp.broadcast_to(row, (128, 128)).T


def turn(matrix):
    return matrix.astype(F32).T.astype(BF16)


def spread_rows(source, scratch, start, groups):
    def step(n, _):
        for part in range(8):
            at = start + n * 8 + part
            scratch[pl.ds(pl.multiple_of(at * PITCH, 8), 32), :] = source[at].astype(F32)
        return _

    lax.fori_loop(0, groups // 8, step, 0)


def each(steps, body):
    def step(j, _):
        body(j)
        return _

    lax.fori_loop(0, steps, step, 0, unroll=8)


def side_by_side(blocks, pair):
    return jnp.concatenate([blocks[pair * 2], blocks[pair * 2 + 1]], axis=1)


def project(normed, weights, hands):
    def body(pair):
        both = side_by_side(normed, pair)
        for side in range(2):
            projected = dot(weights[side * 256 : (side + 1) * 256, :], both)
            hand = sigmoid(projected[0:128]) * projected[128:256]
            for part in range(2):
                at = pl.ds(pl.multiple_of((pair * 2 + part) * WIDE, 8), 128)
                hands[side, at, :] = hand[:, part * 128 : (part + 1) * 128]

    each(16, body)


def gather_hands(hands, send):
    def step(n, _):
        for part in range(8):
            h = n * 8 + part
            for side in range(2):
                send[h, side] = hands[side, pl.ds(h, 32, stride=WIDE), :].astype(BF16)
        return _

    lax.fori_loop(0, 16, step, 0)


def fetch(pairs, arrived):
    copies = [pltpu.make_async_copy(far, near, arrived.at[n]) for n, (far, near) in enumerate(pairs)]
    for copy in copies:
        copy.start()
    return copies


def first_kernel(x, proj, in_gain, send, turned, x_near, proj_near, gain_near, rows, hands, normed, weights, gains, arrived):
    quarters = [pl.ds(n * 32, 32) for n in range(4)]
    pairs = [(x.at[part], x_near.at[part]) for part in quarters]
    pieces = fetch([*pairs, (proj.at[0], proj_near), (in_gain, gain_near)], arrived)
    for n in range(4):
        pieces[n].wait()
        spread_rows(x_near, rows, n * 32, 32)
    pieces[4].wait()
    pieces[5].wait()
    for p in range(4):
        weights[p * 128 : (p + 1) * 128, :] = turn(proj_near[p])
    gains[...] = column(gain_near[0:1, :])

    def body(j):
        channels = rows[pl.ds(j, 128, stride=PITCH), :].T
        turned[j] = channels.astype(BF16)
        normed[j] = layer_norm(channels, gains[...]).astype(BF16)

    each(32, body)
    project(normed, weights, hands)
    gather_hands(hands, send)


def side_kernel(update_index, turned, proj, gate_w, out_w, in_gain, out_gain, gating, out, gains, weights, normed, gate):
    gate[...], out[...] = turn(gate_w[update_index]), turn(out_w[update_index])
    gains[0] = column(out_gain[update_index : update_index + 1, :])
    gains[1] = column(in_gain[1:2, :])
    gains[2] = column(in_gain[update_index : update_index + 1, :])
    for p in range(4):
        weights[p * 128 : (p + 1) * 128, :] = turn(proj[1, p])

    def norm(j):
        normed[j] = layer_norm(turned[j].astype(F32), gains[2]).astype(BF16)

    each(32, norm)

    def body(pair):
        both = sigmoid(dot(gate[...], side_by_side(normed, pair)))
        for part in range(2):
            gating[pair * 2 + part] = both[:, part * 128 : (part + 1) * 128]

    each(16, body)


def mix(tri, mixed, gains):
    def body(j):
        mixed[j] = layer_norm(tri[pl.ds(j, 128, stride=PITCH), :], gains[0]).astype(BF16)

    each(32, body)


def new_channels(turned, gating, mixed, out, pair):
    change = dot(out[...], side_by_side(mixed, pair))
    return [
        turned[pair * 2 + part].astype(F32) + gating[pair * 2 + part] * change[:, part * 128 : (part + 1) * 128]
        for part in range(2)
    ]


def middle_kernel(returned, turned, gating, out, gains, weights, send, newer, tri, hands, mixed, later):
    spread_rows(returned, tri, 0, 128)
    mix(tri, mixed, gains)

    def body(pair):
        for part, channels in enumerate(new_channels(turned, gating, mixed, out, pair)):
            rounded = channels.astype(BF16)
            newer[pair * 2 + part] = rounded
            later[pair * 2 + part] = layer_norm(rounded.astype(F32), gains[1]).astype(BF16)

    each(16, body)
    project(later, weights, hands)
    gather_hands(hands, send)


def last_kernel(returned, turned, gating, out, gains, final, tri, rows, mixed, newer, near, left):
    spread_rows(returned, tri, 0, 128)
    mix(tri, mixed, gains)

    def body(pair):
        for part, channels in enumerate(new_channels(turned, gating, mixed, out, pair)):
            newer[pair * 2 + part] = channels

    each(16, body)

    def back(j):
        rows[pl.ds(j, 128, stride=PITCH), :] = newer[j].T

    each(32, back)
    pieces = []
    for n in range(4):

        def collect(m, _):
            for part in range(8):
                at = n * 32 + m * 8 + part
                near[at] = rows[pl.ds(pl.multiple_of(at * PITCH, 8), 32), :].astype(BF16)
            return _

        lax.fori_loop(0, 4, collect, 0)
        pieces.append(pltpu.make_async_copy(near.at[pl.ds(n * 32, 32)], final.at[pl.ds(n * 32, 32)], left.at[n]))
        pieces[n].start()
    for piece in pieces:
        piece.wait()


def side_of(operands, r, side):
    return operands[r, :, side].reshape(512, 128)


def given_kernel(core, operands, given, kept_rows, lefts, turned):
    for r in range(8):
        lefts[:, r * 128 : (r + 1) * 128] = side_of(operands, r, 0)
        turned[r * 128 : (r + 1) * 128, :] = turn(side_of(operands, r, 1))
    for q in range(16):
        kept_rows[q * 32 : (q + 1) * 32, :] = turned[
            pl.ds(pl.multiple_of(q * 64 + core[0] * 32, 32), 32), :
        ]
    for q in range(0, 16, 4):
        block = jnp.concatenate(
            [turned[pl.ds(pl.multiple_of(p * 64 + 32 - core[0] * 32, 32), 32), :] for p in range(q, q + 4)], axis=0
        )
        product = dot(block, lefts[...]).astype(BF16)
        for r in range(8):
            given[r, q : q + 4] = product[:, r * 128 : (r + 1) * 128].reshape(4, 32, 128)


def kept_kernel(kept_rows, operands, kept):
    lefts = jnp.concatenate([side_of(operands, r, 0) for r in range(8)], axis=1)
    for q in range(0, 16, 4):
        product = dot(kept_rows[q * 32 : (q + 4) * 32, :], lefts)
        for r in range(8):
            kept[r, q : q + 4] = product[:, r * 128 : (r + 1) * 128].reshape(4, 32, 128)


def incoming_kernel(core, operands, other, products, lefts):
    for r in range(8):
        for q in range(16):
            own = pl.multiple_of(q * 64 + core[0] * 32, 32)
            swapped = pl.multiple_of(q * 64 + 32 - core[0] * 32, 32)
            lefts[pl.ds(own, 32), r * 128 : (r + 1) * 128] = operands[r, q, 0]
            lefts[pl.ds(swapped, 32), r * 128 : (r + 1) * 128] = other[r, q]
    rights = jnp.concatenate([side_of(operands, r, 1) for r in range(8)], axis=1)
    for b in range(0, 8, 2):
        product = lax.dot_general(
            rights, lefts[b * 128 : (b + 2) * 128, :], (((1,), (1,)), ((), ())), preferred_element_type=F32
        ).astype(BF16)
        for part in range(2):
            products[b + part] = product[:, part * 128 : (part + 1) * 128].reshape(16, 32, 128)


def shape(dims, kind=BF16):
    return jax.ShapeDtypeStruct(dims, kind)


def call(body, outs, scratch, *args, scalars=0, far=0, far_out=False):
    args = [
        pltpu.with_memory_space_constraint(arg, pltpu.HBM) if scalars <= n < scalars + far else arg
        for n, arg in enumerate(args)
    ]
    vmem, smem, hbm = (pl.BlockSpec(memory_space=space) for space in (pltpu.VMEM, pltpu.SMEM, pltpu.HBM))
    return pl.pallas_call(
        body,
        out_shape=outs,
        in_specs=[smem] * scalars + [hbm] * far + [vmem] * (len(args) - scalars - far),
        out_specs=[hbm if far_out else vmem] * len(outs),
        scratch_shapes=[
            dims if kind is None else pltpu.VMEM(dims, kind) for dims, kind in scratch
        ],
        compiler_params=pltpu.CompilerParams(vmem_limit_bytes=20 * 1024 * 1024),
    )(*args)


def to_chips(pieces):
    return lax.all_to_all(pieces, CHIPS, split_axis=0, concat_axis=0, tiled=True)


ROWS = ((128 * PITCH, 128), F32)
BLOCKS = ((32, 128, 128), BF16)
WHOLE = ((128, 32, 128), BF16)
SQUARE = ((128, 128), BF16)
GAINS = ((3, 128, 128), F32)
HANDS = ((2, 32 * WIDE, 128), F32)
WEIGHTS = ((512, 128), BF16)
SEND = shape((128, 2, 32, 128))
TURNED = shape(*BLOCKS)
HALF = (8, 16, 32, 128)


def first(pair_rep, proj_weight, in_gain):
    near = [WHOLE, ((4, 128, 128), BF16), ((2, 128), F32)]
    scratch = [*near, ROWS, HANDS, BLOCKS, WEIGHTS, ((128, 128), F32), (pltpu.SemaphoreType.DMA((6,)), None)]
    return call(first_kernel, [SEND, TURNED], scratch, pair_rep, proj_weight, in_gain, far=3)


def side(update_index, *args):
    outs = [shape(BLOCKS[0], F32), shape(*SQUARE), shape(*GAINS), shape(*WEIGHTS)]
    body = functools.partial(side_kernel, update_index)
    return call(body, outs, [BLOCKS, SQUARE], *args)


def copies(number):
    return (pltpu.SemaphoreType.DMA((number,)), None)


def middle(returned, turned, gating, out, gains, weights):
    scratch = [ROWS, HANDS, BLOCKS, BLOCKS]
    return call(middle_kernel, [SEND, TURNED], scratch, returned, turned, gating, out, gains, weights)


def last(returned, turned, gating, out, gains):
    scratch = [ROWS, ROWS, BLOCKS, (BLOCKS[0], F32), WHOLE, copies(4)]
    return call(last_kernel, [shape(*WHOLE)], scratch, returned, turned, gating, out, gains, far_out=True)[0]


def exchanged(pieces):
    return lax.ppermute(pieces, "core", SWAP)


def steps(pair_rep, proj_weight, gate_weight, out_weight, in_gain, out_gain):
    core = lax.axis_index("core").astype(jnp.int32).reshape(1)
    core, pair_rep = lax.optimization_barrier((core, pair_rep))
    parameters = (proj_weight, gate_weight, out_weight, in_gain, out_gain)
    send, turned = first(pair_rep, proj_weight, in_gain)
    operands = to_chips(send).reshape(8, 16, 2, 32, 128)
    gating, out, gains, weights = side(0, turned, *parameters)
    given, kept_rows = call(
        given_kernel,
        [shape(HALF), shape((512, 512))],
        [((512, 1024), BF16), ((1024, 512), BF16)],
        core,
        operands,
        scalars=1,
    )
    taken = exchanged(given)
    (kept,) = call(kept_kernel, [shape(HALF, F32)], [], kept_rows, operands)
    triangle = (kept + taken.astype(F32)).astype(BF16)
    returned = to_chips(triangle.reshape(128, 32, 128))
    send, turned = middle(returned, turned, gating, out, gains, weights)
    operands = to_chips(send).reshape(8, 16, 2, 32, 128)
    gating, out, gains, _ = side(1, turned, *parameters)
    other = exchanged(operands[:, :, 0])
    (triangle,) = call(incoming_kernel, [shape(HALF)], [((1024, 1024), BF16)], core, operands, other, scalars=1)
    returned = to_chips(triangle.reshape(128, 32, 128))
    return last(returned, turned, gating, out, gains)


def solution(mesh):
    finer = Mesh(mesh.devices.reshape(8, 16, 2), ("row", "half", "core"))
    placed = (P("row", ("half", "core"), None), P(), P(), P(), P(), P())
    return jax.shard_map(
        steps, mesh=finer, in_specs=placed, out_specs=P("row", ("half", "core"), None), check_vma=False
    )
```

```python
import functools

import jax
import jax.numpy as jnp
from jax import lax
from jax.experimental import pallas as pl
from jax.experimental.pallas import tpu as pltpu
from jax.sharding import Mesh
from jax.sharding import PartitionSpec as P


CHIPS = ("row", "half")
SWAP = [(0, 1), (1, 0)]
F32 = jnp.float32
BF16 = jnp.bfloat16
PITCH = 40
WIDE = 136
STAGGER = 3100


epsilon = 1e-05


def dot(a, b):
    return lax.dot_general(a, b, (((1,), (0,)), ((), ())), preferred_element_type=F32)


def sigmoid(values):
    return 0.5 * jnp.tanh(0.5 * values) + 0.5


def layer_norm(values, gain):
    center = values - jnp.sum(values, axis=0, keepdims=True) * (1.0 / 128)
    spread = jnp.sum(center * center, axis=0, keepdims=True) * (1.0 / 128)
    return center * lax.rsqrt(spread + epsilon) * gain


def column(row):
    return jnp.broadcast_to(row, (128, 128)).T


def turn(matrix):
    return matrix.astype(F32).T.astype(BF16)


def spread_rows(source, scratch, start, groups):
    def step(n, _):
        for part in range(8):
            at = start + n * 8 + part
            scratch[pl.ds(pl.multiple_of(at * PITCH, 8), 32), :] = source[at].astype(F32)
        return _

    lax.fori_loop(0, groups // 8, step, 0)


def each(steps, body):
    def step(j, _):
        body(j)
        return _

    lax.fori_loop(0, steps, step, 0, unroll=8)


def side_by_side(blocks, pair):
    return jnp.concatenate([blocks[pair * 2], blocks[pair * 2 + 1]], axis=1)


def project(normed, weights, hands):
    def body(pair):
        both = side_by_side(normed, pair)
        for side in range(2):
            projected = dot(weights[side * 256 : (side + 1) * 256, :], both)
            hand = sigmoid(projected[0:128]) * projected[128:256]
            for part in range(2):
                at = pl.ds(pl.multiple_of((pair * 2 + part) * WIDE, 8), 128)
                hands[side, at, :] = hand[:, part * 128 : (part + 1) * 128]

    each(16, body)


def gather_hands(hands, send):
    def step(n, _):
        for part in range(8):
            h = n * 8 + part
            for side in range(2):
                send[h, side] = hands[side, pl.ds(h, 32, stride=WIDE), :].astype(BF16)
        return _

    lax.fori_loop(0, 16, step, 0)


def fetch(pairs, arrived):
    copies = [pltpu.make_async_copy(far, near, arrived.at[n]) for n, (far, near) in enumerate(pairs)]
    for copy in copies:
        copy.start()
    return copies


def first_kernel(x, proj, in_gain, send, turned, x_near, proj_near, gain_near, rows, hands, normed, weights, gains, arrived):
    quarters = [pl.ds(n * 32, 32) for n in range(4)]
    pairs = [(x.at[part], x_near.at[part]) for part in quarters]
    pieces = fetch([*pairs, (proj.at[0], proj_near), (in_gain, gain_near)], arrived)
    for n in range(4):
        pieces[n].wait()
        spread_rows(x_near, rows, n * 32, 32)
    pieces[4].wait()
    pieces[5].wait()
    for p in range(4):
        weights[p * 128 : (p + 1) * 128, :] = turn(proj_near[p])
    gains[...] = column(gain_near[0:1, :])

    def body(j):
        channels = rows[pl.ds(j, 128, stride=PITCH), :].T
        turned[j] = channels.astype(BF16)
        normed[j] = layer_norm(channels, gains[...]).astype(BF16)

    each(32, body)
    project(normed, weights, hands)
    gather_hands(hands, send)


def side_kernel(update_index, turned, proj, gate_w, out_w, in_gain, out_gain, gating, out, gains, weights, normed, gate):
    gate[...], out[...] = turn(gate_w[update_index]), turn(out_w[update_index])
    gains[0] = column(out_gain[update_index : update_index + 1, :])
    gains[1] = column(in_gain[1:2, :])
    gains[2] = column(in_gain[update_index : update_index + 1, :])
    for p in range(4):
        weights[p * 128 : (p + 1) * 128, :] = turn(proj[1, p])

    def norm(j):
        normed[j] = layer_norm(turned[j].astype(F32), gains[2]).astype(BF16)

    each(32, norm)

    def body(pair):
        both = sigmoid(dot(gate[...], side_by_side(normed, pair)))
        for part in range(2):
            gating[pair * 2 + part] = both[:, part * 128 : (part + 1) * 128]

    each(16, body)


def mix(tri, mixed, gains):
    def body(j):
        mixed[j] = layer_norm(tri[pl.ds(j, 128, stride=PITCH), :], gains[0]).astype(BF16)

    each(32, body)


def new_channels(turned, gating, mixed, out, pair):
    change = dot(out[...], side_by_side(mixed, pair))
    return [
        turned[pair * 2 + part].astype(F32) + gating[pair * 2 + part] * change[:, part * 128 : (part + 1) * 128]
        for part in range(2)
    ]


def middle_kernel(returned, turned, gating, out, gains, weights, send, newer, tri, hands, mixed, later):
    spread_rows(returned, tri, 0, 128)
    mix(tri, mixed, gains)

    def body(pair):
        for part, channels in enumerate(new_channels(turned, gating, mixed, out, pair)):
            rounded = channels.astype(BF16)
            newer[pair * 2 + part] = rounded
            later[pair * 2 + part] = layer_norm(rounded.astype(F32), gains[1]).astype(BF16)

    each(16, body)
    project(later, weights, hands)
    gather_hands(hands, send)


def last_kernel(returned, turned, gating, out, gains, final, tri, rows, mixed, newer, near, left):
    spread_rows(returned, tri, 0, 128)
    mix(tri, mixed, gains)

    def body(pair):
        for part, channels in enumerate(new_channels(turned, gating, mixed, out, pair)):
            newer[pair * 2 + part] = channels

    each(16, body)

    def back(j):
        rows[pl.ds(j, 128, stride=PITCH), :] = newer[j].T

    each(32, back)
    pieces = []
    for n in range(4):

        def collect(m, _):
            for part in range(8):
                at = n * 32 + m * 8 + part
                near[at] = rows[pl.ds(pl.multiple_of(at * PITCH, 8), 32), :].astype(BF16)
            return _

        lax.fori_loop(0, 4, collect, 0)
        pieces.append(pltpu.make_async_copy(near.at[pl.ds(n * 32, 32)], final.at[pl.ds(n * 32, 32)], left.at[n]))
        pieces[n].start()
    for piece in pieces:
        piece.wait()


def side_of(operands, r, side):
    return operands[r, :, side].reshape(512, 128)


def given_kernel(core, operands, given, kept_rows, lefts, turned):
    for r in range(8):
        lefts[:, r * 128 : (r + 1) * 128] = side_of(operands, r, 0)
        turned[r * 128 : (r + 1) * 128, :] = turn(side_of(operands, r, 1))
    for q in range(16):
        kept_rows[q * 32 : (q + 1) * 32, :] = turned[
            pl.ds(pl.multiple_of(q * 64 + core[0] * 32, 32), 32), :
        ]
    for q in range(0, 16, 4):
        block = jnp.concatenate(
            [turned[pl.ds(pl.multiple_of(p * 64 + 32 - core[0] * 32, 32), 32), :] for p in range(q, q + 4)], axis=0
        )
        product = dot(block, lefts[...]).astype(BF16)
        for r in range(8):
            given[r, q : q + 4] = product[:, r * 128 : (r + 1) * 128].reshape(4, 32, 128)


def kept_kernel(kept_rows, operands, kept):
    lefts = jnp.concatenate([side_of(operands, r, 0) for r in range(8)], axis=1)
    for q in range(0, 16, 4):
        product = dot(kept_rows[q * 32 : (q + 4) * 32, :], lefts)
        for r in range(8):
            kept[r, q : q + 4] = product[:, r * 128 : (r + 1) * 128].reshape(4, 32, 128)


def joined_kernel(core, kept, taken, joined, spun):
    spun[...] = lax.fori_loop(0, core[0] * STAGGER, lambda _, a: a * 0.5 + 0.25, jnp.ones((8, 128), F32))
    for r in range(8):
        joined[r] = (kept[r] + taken[r].astype(F32)).astype(BF16)


def incoming_kernel(core, operands, other, products, lefts):
    for r in range(8):
        for q in range(16):
            own = pl.multiple_of(q * 64 + core[0] * 32, 32)
            swapped = pl.multiple_of(q * 64 + 32 - core[0] * 32, 32)
            lefts[pl.ds(own, 32), r * 128 : (r + 1) * 128] = operands[r, q, 0]
            lefts[pl.ds(swapped, 32), r * 128 : (r + 1) * 128] = other[r, q]
    rights = jnp.concatenate([side_of(operands, r, 1) for r in range(8)], axis=1)
    for b in range(0, 8, 2):
        product = lax.dot_general(
            rights, lefts[b * 128 : (b + 2) * 128, :], (((1,), (1,)), ((), ())), preferred_element_type=F32
        ).astype(BF16)
        for part in range(2):
            products[b + part] = product[:, part * 128 : (part + 1) * 128].reshape(16, 32, 128)


def shape(dims, kind=BF16):
    return jax.ShapeDtypeStruct(dims, kind)


def call(body, outs, scratch, *args, scalars=0, far=0, far_out=False):
    args = [
        pltpu.with_memory_space_constraint(arg, pltpu.HBM) if scalars <= n < scalars + far else arg
        for n, arg in enumerate(args)
    ]
    vmem, smem, hbm = (pl.BlockSpec(memory_space=space) for space in (pltpu.VMEM, pltpu.SMEM, pltpu.HBM))
    return pl.pallas_call(
        body,
        out_shape=outs,
        in_specs=[smem] * scalars + [hbm] * far + [vmem] * (len(args) - scalars - far),
        out_specs=[hbm if far_out else vmem] * len(outs),
        scratch_shapes=[
            dims if kind is None else pltpu.VMEM(dims, kind) for dims, kind in scratch
        ],
        compiler_params=pltpu.CompilerParams(vmem_limit_bytes=20 * 1024 * 1024),
    )(*args)


def to_chips(pieces):
    return lax.all_to_all(pieces, CHIPS, split_axis=0, concat_axis=0, tiled=True)


ROWS = ((128 * PITCH, 128), F32)
BLOCKS = ((32, 128, 128), BF16)
WHOLE = ((128, 32, 128), BF16)
SQUARE = ((128, 128), BF16)
GAINS = ((3, 128, 128), F32)
HANDS = ((2, 32 * WIDE, 128), F32)
WEIGHTS = ((512, 128), BF16)
SEND = shape((128, 2, 32, 128))
TURNED = shape(*BLOCKS)
HALF = (8, 16, 32, 128)


def first(pair_rep, proj_weight, in_gain):
    near = [WHOLE, ((4, 128, 128), BF16), ((2, 128), F32)]
    scratch = [*near, ROWS, HANDS, BLOCKS, WEIGHTS, ((128, 128), F32), (pltpu.SemaphoreType.DMA((6,)), None)]
    return call(first_kernel, [SEND, TURNED], scratch, pair_rep, proj_weight, in_gain, far=3)


def side(update_index, *args):
    outs = [shape(BLOCKS[0], F32), shape(*SQUARE), shape(*GAINS), shape(*WEIGHTS)]
    body = functools.partial(side_kernel, update_index)
    return call(body, outs, [BLOCKS, SQUARE], *args)


def copies(number):
    return (pltpu.SemaphoreType.DMA((number,)), None)


def middle(returned, turned, gating, out, gains, weights):
    scratch = [ROWS, HANDS, BLOCKS, BLOCKS]
    return call(middle_kernel, [SEND, TURNED], scratch, returned, turned, gating, out, gains, weights)


def last(returned, turned, gating, out, gains):
    scratch = [ROWS, ROWS, BLOCKS, (BLOCKS[0], F32), WHOLE, copies(4)]
    return call(last_kernel, [shape(*WHOLE)], scratch, returned, turned, gating, out, gains, far_out=True)[0]


def exchanged(pieces):
    return lax.ppermute(pieces, "core", SWAP)


def steps(pair_rep, proj_weight, gate_weight, out_weight, in_gain, out_gain):
    core = lax.axis_index("core").astype(jnp.int32).reshape(1)
    core, pair_rep = lax.optimization_barrier((core, pair_rep))
    parameters = (proj_weight, gate_weight, out_weight, in_gain, out_gain)
    send, turned = first(pair_rep, proj_weight, in_gain)
    operands = to_chips(send).reshape(8, 16, 2, 32, 128)
    gating, out, gains, weights = side(0, turned, *parameters)
    given, kept_rows = call(
        given_kernel,
        [shape(HALF), shape((512, 512))],
        [((512, 1024), BF16), ((1024, 512), BF16)],
        core,
        operands,
        scalars=1,
    )
    taken = exchanged(given)
    (kept,) = call(kept_kernel, [shape(HALF, F32)], [], kept_rows, operands)
    triangle, _ = call(joined_kernel, [shape(HALF), shape((8, 128), F32)], [], core, kept, taken, scalars=1)
    returned = to_chips(triangle.reshape(128, 32, 128))
    send, turned = middle(returned, turned, gating, out, gains, weights)
    operands = to_chips(send).reshape(8, 16, 2, 32, 128)
    gating, out, gains, _ = side(1, turned, *parameters)
    other = exchanged(operands[:, :, 0])
    (triangle,) = call(incoming_kernel, [shape(HALF)], [((1024, 1024), BF16)], core, operands, other, scalars=1)
    returned = to_chips(triangle.reshape(128, 32, 128))
    return last(returned, turned, gating, out, gains)


def solution(mesh):
    finer = Mesh(mesh.devices.reshape(8, 16, 2), ("row", "half", "core"))
    placed = (P("row", ("half", "core"), None), P(), P(), P(), P(), P())
    return jax.shard_map(
        steps, mesh=finer, in_specs=placed, out_specs=P("row", ("half", "core"), None), check_vma=False
    )
```

```python
import functools

import jax
import jax.numpy as jnp
from jax import lax
from jax.experimental import pallas as pl
from jax.experimental.pallas import tpu as pltpu
from jax.sharding import Mesh
from jax.sharding import PartitionSpec as P


CHIPS = ("row", "half")
SWAP = [(0, 1), (1, 0)]
F32 = jnp.float32
BF16 = jnp.bfloat16
PITCH = 40
WIDE = 136
STAGGER = 2600


epsilon = 1e-05


def dot(a, b):
    return lax.dot_general(a, b, (((1,), (0,)), ((), ())), preferred_element_type=F32)


def sigmoid(values):
    return 0.5 * jnp.tanh(0.5 * values) + 0.5


def layer_norm(values, gain):
    center = values - jnp.sum(values, axis=0, keepdims=True) * (1.0 / 128)
    spread = jnp.sum(center * center, axis=0, keepdims=True) * (1.0 / 128)
    return center * lax.rsqrt(spread + epsilon) * gain


def column(row):
    return jnp.broadcast_to(row, (128, 128)).T


def turn(matrix):
    return matrix.astype(F32).T.astype(BF16)


def spread_rows(source, scratch, start, groups):
    def step(n, _):
        for part in range(8):
            at = start + n * 8 + part
            scratch[pl.ds(pl.multiple_of(at * PITCH, 8), 32), :] = source[at].astype(F32)
        return _

    lax.fori_loop(0, groups // 8, step, 0)


def each(steps, body):
    def step(j, _):
        body(j)
        return _

    lax.fori_loop(0, steps, step, 0, unroll=8)


def side_by_side(blocks, pair):
    return jnp.concatenate([blocks[pair * 2], blocks[pair * 2 + 1]], axis=1)


def project(normed, weights, hands):
    def body(pair):
        both = side_by_side(normed, pair)
        for side in range(2):
            projected = dot(weights[side * 256 : (side + 1) * 256, :], both)
            hand = sigmoid(projected[0:128]) * projected[128:256]
            for part in range(2):
                at = pl.ds(pl.multiple_of((pair * 2 + part) * WIDE, 8), 128)
                hands[side, at, :] = hand[:, part * 128 : (part + 1) * 128]

    each(16, body)


def gather_side(hands, side, target, start, number):
    def step(n, _):
        for part in range(8):
            h = start + n * 8 + part
            target[h] = hands[side, pl.ds(h, 32, stride=WIDE), :].astype(BF16)
        return _

    lax.fori_loop(0, number // 8, step, 0)


def fetch(pairs, arrived):
    copies = [pltpu.make_async_copy(far, near, arrived.at[n]) for n, (far, near) in enumerate(pairs)]
    for copy in copies:
        copy.start()
    return copies


def first_kernel(x, proj, in_gain, send, turned, x_near, proj_near, gain_near, rows, hands, normed, weights, gains, arrived):
    quarters = [pl.ds(n * 32, 32) for n in range(4)]
    pairs = [(x.at[part], x_near.at[part]) for part in quarters]
    pieces = fetch([(proj.at[0], proj_near), (in_gain, gain_near), *pairs], arrived)
    pieces[0].wait()
    pieces[1].wait()
    for p in range(4):
        weights[p * 128 : (p + 1) * 128, :] = turn(proj_near[p])
    gains[...] = column(gain_near[0:1, :])
    for n in range(4):
        pieces[2 + n].wait()
        spread_rows(x_near, rows, n * 32, 32)

    def body(j):
        channels = rows[pl.ds(j, 128, stride=PITCH), :].T
        turned[j] = channels.astype(BF16)
        normed[j] = layer_norm(channels, gains[...]).astype(BF16)

    each(32, body)
    project(normed, weights, hands)
    for side in range(2):
        gather_side(hands, side, send.at[:, side], 0, 128)


def side_kernel(update_index, turned, proj, gate_w, out_w, in_gain, out_gain, gating, out, gains, weights, normed, gate):
    gate[...], out[...] = turn(gate_w[update_index]), turn(out_w[update_index])
    gains[0] = column(out_gain[update_index : update_index + 1, :])
    gains[1] = column(in_gain[1:2, :])
    gains[2] = column(in_gain[update_index : update_index + 1, :])
    for p in range(4):
        weights[p * 128 : (p + 1) * 128, :] = turn(proj[1, p])

    def norm(j):
        normed[j] = layer_norm(turned[j].astype(F32), gains[2]).astype(BF16)

    each(32, norm)

    def body(pair):
        both = sigmoid(dot(gate[...], side_by_side(normed, pair)))
        for part in range(2):
            gating[pair * 2 + part] = both[:, part * 128 : (part + 1) * 128]

    each(16, body)


def mix(tri, mixed, gains):
    def body(j):
        mixed[j] = layer_norm(tri[pl.ds(j, 128, stride=PITCH), :], gains[0]).astype(BF16)

    each(32, body)


def new_channels(turned, gating, mixed, out, pair):
    change = dot(out[...], side_by_side(mixed, pair))
    return [
        turned[pair * 2 + part].astype(F32) + gating[pair * 2 + part] * change[:, part * 128 : (part + 1) * 128]
        for part in range(2)
    ]


def middle_kernel(returned, turned, gating, out, gains, weights, left, right, newer, tri, hands, mixed, later, right_near, leaving):
    spread_rows(returned, tri, 0, 128)
    mix(tri, mixed, gains)

    def body(pair):
        for part, channels in enumerate(new_channels(turned, gating, mixed, out, pair)):
            rounded = channels.astype(BF16)
            newer[pair * 2 + part] = rounded
            later[pair * 2 + part] = layer_norm(rounded.astype(F32), gains[1]).astype(BF16)

    each(16, body)
    project(later, weights, hands)
    pieces = []
    for n in range(2):
        part = pl.ds(n * 64, 64)
        gather_side(hands, 1, right_near, n * 64, 64)
        pieces.append(pltpu.make_async_copy(right_near.at[part], right.at[part], leaving.at[n]))
        pieces[n].start()
    gather_side(hands, 0, left, 0, 128)
    for piece in pieces:
        piece.wait()


def last_kernel(
    far_gains, far_out, far_gating, far_turned, returned, final,
    gains, out, gating, turned, tri, rows, mixed, newer, near, arrived, left,
):
    halves = [pl.ds(0, 16), pl.ds(16, 16)]
    pairs = [(far_gains, gains), (far_out, out)]
    for part in halves:
        pairs += [(far_gating.at[part], gating.at[part]), (far_turned.at[part], turned.at[part])]
    pieces = fetch(pairs, arrived)
    spread_rows(returned, tri, 0, 128)
    pieces[0].wait()
    mix(tri, mixed, gains)
    pieces[1].wait()

    def body(pair):
        for part, channels in enumerate(new_channels(turned, gating, mixed, out, pair)):
            newer[pair * 2 + part] = channels

    for n in range(2):
        pieces[2 + 2 * n].wait()
        pieces[3 + 2 * n].wait()
        each(8, lambda pair, n=n: body(n * 8 + pair))

    def back(j):
        rows[pl.ds(j, 128, stride=PITCH), :] = newer[j].T

    each(32, back)
    pieces = []
    for n in range(4):

        def collect(m, _):
            for part in range(8):
                at = n * 32 + m * 8 + part
                near[at] = rows[pl.ds(pl.multiple_of(at * PITCH, 8), 32), :].astype(BF16)
            return _

        lax.fori_loop(0, 4, collect, 0)
        pieces.append(pltpu.make_async_copy(near.at[pl.ds(n * 32, 32)], final.at[pl.ds(n * 32, 32)], left.at[n]))
        pieces[n].start()
    for piece in pieces:
        piece.wait()


def side_of(operands, r, side):
    return operands[r, :, side].reshape(512, 128)


def given_kernel(core, operands, given, kept_rows, lefts, turned):
    for r in range(8):
        lefts[:, r * 128 : (r + 1) * 128] = side_of(operands, r, 0)
        turned[r * 128 : (r + 1) * 128, :] = turn(side_of(operands, r, 1))
    for q in range(16):
        kept_rows[q * 32 : (q + 1) * 32, :] = turned[
            pl.ds(pl.multiple_of(q * 64 + core[0] * 32, 32), 32), :
        ]
    for q in range(0, 16, 4):
        block = jnp.concatenate(
            [turned[pl.ds(pl.multiple_of(p * 64 + 32 - core[0] * 32, 32), 32), :] for p in range(q, q + 4)], axis=0
        )
        product = dot(block, lefts[...]).astype(BF16)
        for r in range(8):
            given[r, q : q + 4] = product[:, r * 128 : (r + 1) * 128].reshape(4, 32, 128)


def kept_kernel(kept_rows, operands, kept):
    lefts = jnp.concatenate([side_of(operands, r, 0) for r in range(8)], axis=1)
    for q in range(0, 16, 4):
        product = dot(kept_rows[q * 32 : (q + 4) * 32, :], lefts)
        for r in range(8):
            kept[r, q : q + 4] = product[:, r * 128 : (r + 1) * 128].reshape(4, 32, 128)


def joined_kernel(core, kept, taken, joined, spun):
    spun[...] = lax.fori_loop(0, core[0] * STAGGER, lambda _, a: a * 0.5 + 0.25, jnp.ones((8, 128), F32))
    for r in range(8):
        joined[r] = (kept[r] + taken[r].astype(F32)).astype(BF16)


def incoming_kernel(core, own, other, operand, products, lefts, arrived):
    pairs = []
    for q in (0, 8):
        for r in range(8):
            lanes = pl.ds(r * 128, 128)
            pairs.append((own.at[r, pl.ds(q, 8)], lefts.at[pl.ds(q, 8), core[0], :, lanes]))
            pairs.append((other.at[r, pl.ds(q, 8)], lefts.at[pl.ds(q, 8), 1 - core[0], :, lanes]))
    pieces = fetch(pairs, arrived)
    rights = jnp.concatenate([operand[r].reshape(512, 128) for r in range(8)], axis=1)
    for b in range(0, 8, 2):
        if b % 4 == 0:
            for piece in pieces[b * 4 : b * 4 + 16]:
                piece.wait()
        product = lax.dot_general(
            rights,
            lefts[b * 2 : b * 2 + 4].reshape(256, 1024),
            (((1,), (1,)), ((), ())),
            preferred_element_type=F32,
        ).astype(BF16)
        for part in range(2):
            products[b + part] = product[:, part * 128 : (part + 1) * 128].reshape(16, 32, 128)


def shape(dims, kind=BF16):
    return jax.ShapeDtypeStruct(dims, kind)


def call(body, outs, scratch, *args, scalars=0, far=0, far_outs=()):
    args = [
        pltpu.with_memory_space_constraint(arg, pltpu.HBM) if scalars <= n < scalars + far else arg
        for n, arg in enumerate(args)
    ]
    vmem, smem, hbm = (pl.BlockSpec(memory_space=space) for space in (pltpu.VMEM, pltpu.SMEM, pltpu.HBM))
    return pl.pallas_call(
        body,
        out_shape=outs,
        in_specs=[smem] * scalars + [hbm] * far + [vmem] * (len(args) - scalars - far),
        out_specs=[hbm if n in far_outs else vmem for n in range(len(outs))],
        scratch_shapes=[
            dims if kind is None else pltpu.VMEM(dims, kind) for dims, kind in scratch
        ],
        compiler_params=pltpu.CompilerParams(vmem_limit_bytes=20 * 1024 * 1024),
    )(*args)


def to_chips(pieces):
    return lax.all_to_all(pieces, CHIPS, split_axis=0, concat_axis=0, tiled=True)


ROWS = ((128 * PITCH, 128), F32)
BLOCKS = ((32, 128, 128), BF16)
WHOLE = ((128, 32, 128), BF16)
SQUARE = ((128, 128), BF16)
GAINS = ((3, 128, 128), F32)
HANDS = ((2, 32 * WIDE, 128), F32)
WEIGHTS = ((512, 128), BF16)
SEND = shape((128, 2, 32, 128))
TURNED = shape(*BLOCKS)
HALF = (8, 16, 32, 128)


def first(pair_rep, proj_weight, in_gain):
    near = [WHOLE, ((4, 128, 128), BF16), ((2, 128), F32)]
    scratch = [*near, ROWS, HANDS, BLOCKS, WEIGHTS, ((128, 128), F32), (pltpu.SemaphoreType.DMA((6,)), None)]
    return call(first_kernel, [SEND, TURNED], scratch, pair_rep, proj_weight, in_gain, far=3)


def side(update_index, *args):
    outs = [shape(BLOCKS[0], F32), shape(*SQUARE), shape(*GAINS), shape(*WEIGHTS)]
    body = functools.partial(side_kernel, update_index)
    return call(body, outs, [BLOCKS, SQUARE], *args)


def copies(number):
    return (pltpu.SemaphoreType.DMA((number,)), None)


def middle(returned, turned, gating, out, gains, weights):
    scratch = [ROWS, HANDS, BLOCKS, BLOCKS, WHOLE, copies(2)]
    outs = [shape(*WHOLE), pltpu.HBM(*WHOLE), TURNED]
    return call(middle_kernel, outs, scratch, returned, turned, gating, out, gains, weights, far_outs=(1,))


def last(returned, turned, gating, out, gains):
    near = [GAINS, SQUARE, (BLOCKS[0], F32), BLOCKS]
    scratch = [*near, ROWS, ROWS, BLOCKS, (BLOCKS[0], F32), WHOLE, copies(6), copies(4)]
    return call(last_kernel, [shape(*WHOLE)], scratch, gains, out, gating, turned, returned, far=4, far_outs=(0,))[0]


def exchanged(pieces):
    return lax.ppermute(pieces, "core", SWAP)


def steps(pair_rep, proj_weight, gate_weight, out_weight, in_gain, out_gain):
    core = lax.axis_index("core").astype(jnp.int32).reshape(1)
    core, pair_rep = lax.optimization_barrier((core, pair_rep))
    parameters = (proj_weight, gate_weight, out_weight, in_gain, out_gain)
    send, turned = first(pair_rep, proj_weight, in_gain)
    operands = to_chips(send).reshape(8, 16, 2, 32, 128)
    gating, out, gains, weights = side(0, turned, *parameters)
    given, kept_rows = call(
        given_kernel,
        [shape(HALF), shape((512, 512))],
        [((512, 1024), BF16), ((1024, 512), BF16)],
        core,
        operands,
        scalars=1,
    )
    taken = exchanged(given)
    (kept,) = call(kept_kernel, [shape(HALF, F32)], [], kept_rows, operands)
    triangle, _ = call(joined_kernel, [shape(HALF), shape((8, 128), F32)], [], core, kept, taken, scalars=1)
    returned = to_chips(triangle.reshape(128, 32, 128))
    left, right, turned = middle(returned, turned, gating, out, gains, weights)
    left = to_chips(left).reshape(HALF)
    right = to_chips(right).reshape(HALF)
    gating, out, gains, _ = side(1, turned, *parameters)
    other = exchanged(left)
    (triangle,) = call(
        incoming_kernel,
        [shape(HALF)],
        [((16, 2, 32, 1024), BF16), copies(32)],
        core,
        left,
        other,
        right,
        scalars=1,
        far=2,
    )
    returned = to_chips(triangle.reshape(128, 32, 128))
    return last(returned, turned, gating, out, gains)


def solution(mesh):
    finer = Mesh(mesh.devices.reshape(8, 16, 2), ("row", "half", "core"))
    placed = (P("row", ("half", "core"), None), P(), P(), P(), P(), P())
    return jax.shard_map(
        steps, mesh=finer, in_specs=placed, out_specs=P("row", ("half", "core"), None), check_vma=False
    )
```

```python
import functools

import jax
import jax.numpy as jnp
from jax import lax
from jax.experimental import pallas as pl
from jax.experimental.pallas import tpu as pltpu
from jax.sharding import Mesh
from jax.sharding import PartitionSpec as P


CHIPS = ("row", "half")
SWAP = [(0, 1), (1, 0)]
F32 = jnp.float32
BF16 = jnp.bfloat16
PITCH = 40
WIDE = 136
STAGGER = 2750


epsilon = 1e-05


def dot(a, b):
    return lax.dot_general(a, b, (((1,), (0,)), ((), ())), preferred_element_type=F32)


def sigmoid(values):
    return 0.5 * jnp.tanh(0.5 * values) + 0.5


def layer_norm(values, gain):
    center = values - jnp.sum(values, axis=0, keepdims=True) * (1.0 / 128)
    spread = jnp.sum(center * center, axis=0, keepdims=True) * (1.0 / 128)
    return center * lax.rsqrt(spread + epsilon) * gain


def column(row):
    return jnp.broadcast_to(row, (128, 128)).T


def turn(matrix):
    return matrix.astype(F32).T.astype(BF16)


def spread_rows(source, scratch, start, groups):
    def step(n, _):
        for part in range(8):
            at = start + n * 8 + part
            scratch[pl.ds(pl.multiple_of(at * PITCH, 8), 32), :] = source[at].astype(F32)
        return _

    lax.fori_loop(0, groups // 8, step, 0)


def each(steps, body):
    def step(j, _):
        body(j)
        return _

    lax.fori_loop(0, steps, step, 0, unroll=8)


def side_by_side(blocks, pair):
    return jnp.concatenate([blocks[pair * 2], blocks[pair * 2 + 1]], axis=1)


def project(normed, weights, hands):
    def body(pair):
        both = side_by_side(normed, pair)
        for side in range(2):
            projected = dot(weights[side * 256 : (side + 1) * 256, :], both)
            hand = sigmoid(projected[0:128]) * projected[128:256]
            for part in range(2):
                at = pl.ds(pl.multiple_of((pair * 2 + part) * WIDE, 8), 128)
                hands[side, at, :] = hand[:, part * 128 : (part + 1) * 128]

    each(16, body)


def gather_side(hands, side, target, start, number):
    def step(n, _):
        for part in range(8):
            h = start + n * 8 + part
            target[h] = hands[side, pl.ds(h, 32, stride=WIDE), :].astype(BF16)
        return _

    lax.fori_loop(0, number // 8, step, 0)


def fetch(pairs, arrived):
    copies = [pltpu.make_async_copy(far, near, arrived.at[n]) for n, (far, near) in enumerate(pairs)]
    for copy in copies:
        copy.start()
    return copies


def first_kernel(x, proj, in_gain, send, turned, x_near, proj_near, gain_near, rows, hands, normed, weights, gains, arrived):
    quarters = [pl.ds(n * 32, 32) for n in range(4)]
    pairs = [(x.at[part], x_near.at[part]) for part in quarters]
    pieces = fetch([(proj.at[0], proj_near), (in_gain, gain_near), *pairs], arrived)
    pieces[0].wait()
    pieces[1].wait()
    for p in range(4):
        weights[p * 128 : (p + 1) * 128, :] = turn(proj_near[p])
    gains[...] = column(gain_near[0:1, :])
    for n in range(4):
        pieces[2 + n].wait()
        spread_rows(x_near, rows, n * 32, 32)

    def body(j):
        channels = rows[pl.ds(j, 128, stride=PITCH), :].T
        turned[j] = channels.astype(BF16)
        normed[j] = layer_norm(channels, gains[...]).astype(BF16)

    each(32, body)
    project(normed, weights, hands)
    for side in range(2):
        gather_side(hands, side, send.at[:, side], 0, 128)


def side_kernel(update_index, turned, proj, gate_w, out_w, in_gain, out_gain, gating, out, gains, weights, normed, gate):
    gate[...], out[...] = turn(gate_w[update_index]), turn(out_w[update_index])
    gains[0] = column(out_gain[update_index : update_index + 1, :])
    gains[1] = column(in_gain[1:2, :])
    gains[2] = column(in_gain[update_index : update_index + 1, :])
    for p in range(4):
        weights[p * 128 : (p + 1) * 128, :] = turn(proj[1, p])

    def norm(j):
        normed[j] = layer_norm(turned[j].astype(F32), gains[2]).astype(BF16)

    each(32, norm)

    def body(pair):
        both = sigmoid(dot(gate[...], side_by_side(normed, pair)))
        for part in range(2):
            gating[pair * 2 + part] = both[:, part * 128 : (part + 1) * 128]

    each(16, body)


def mix(tri, mixed, gains):
    def body(j):
        mixed[j] = layer_norm(tri[pl.ds(j, 128, stride=PITCH), :], gains[0]).astype(BF16)

    each(32, body)


def new_channels(turned, gating, mixed, out, pair):
    change = dot(out[...], side_by_side(mixed, pair))
    return [
        turned[pair * 2 + part].astype(F32) + gating[pair * 2 + part] * change[:, part * 128 : (part + 1) * 128]
        for part in range(2)
    ]


def middle_kernel(returned, turned, gating, out, gains, weights, left, right, newer, tri, hands, mixed, later, right_near, leaving):
    spread_rows(returned, tri, 0, 128)
    mix(tri, mixed, gains)

    def body(pair):
        for part, channels in enumerate(new_channels(turned, gating, mixed, out, pair)):
            rounded = channels.astype(BF16)
            newer[pair * 2 + part] = rounded
            later[pair * 2 + part] = layer_norm(rounded.astype(F32), gains[1]).astype(BF16)

    each(16, body)
    project(later, weights, hands)
    pieces = []
    for n in range(2):
        part = pl.ds(n * 64, 64)
        gather_side(hands, 1, right_near, n * 64, 64)
        pieces.append(pltpu.make_async_copy(right_near.at[part], right.at[part], leaving.at[n]))
        pieces[n].start()
    gather_side(hands, 0, left, 0, 128)
    for piece in pieces:
        piece.wait()


def last_kernel(returned, turned, gating, out, gains, final, tri, rows, mixed, newer, near, left):
    spread_rows(returned, tri, 0, 128)
    mix(tri, mixed, gains)

    def body(pair):
        for part, channels in enumerate(new_channels(turned, gating, mixed, out, pair)):
            newer[pair * 2 + part] = channels

    each(16, body)

    def back(j):
        rows[pl.ds(j, 128, stride=PITCH), :] = newer[j].T

    each(32, back)
    pieces = []
    for n in range(4):

        def collect(m, _):
            for part in range(8):
                at = n * 32 + m * 8 + part
                near[at] = rows[pl.ds(pl.multiple_of(at * PITCH, 8), 32), :].astype(BF16)
            return _

        lax.fori_loop(0, 4, collect, 0)
        pieces.append(pltpu.make_async_copy(near.at[pl.ds(n * 32, 32)], final.at[pl.ds(n * 32, 32)], left.at[n]))
        pieces[n].start()
    for piece in pieces:
        piece.wait()


def side_of(operands, r, side):
    return operands[r, :, side].reshape(512, 128)


def given_kernel(core, operands, given, kept_rows, lefts, turned):
    for r in range(8):
        lefts[:, r * 128 : (r + 1) * 128] = side_of(operands, r, 0)
        turned[r * 128 : (r + 1) * 128, :] = turn(side_of(operands, r, 1))
    for q in range(16):
        kept_rows[q * 32 : (q + 1) * 32, :] = turned[
            pl.ds(pl.multiple_of(q * 64 + core[0] * 32, 32), 32), :
        ]
    for q in range(0, 16, 4):
        block = jnp.concatenate(
            [turned[pl.ds(pl.multiple_of(p * 64 + 32 - core[0] * 32, 32), 32), :] for p in range(q, q + 4)], axis=0
        )
        product = dot(block, lefts[...]).astype(BF16)
        for r in range(8):
            given[r, q : q + 4] = product[:, r * 128 : (r + 1) * 128].reshape(4, 32, 128)


def kept_kernel(kept_rows, operands, kept):
    lefts = jnp.concatenate([side_of(operands, r, 0) for r in range(8)], axis=1)
    for q in range(0, 16, 4):
        product = dot(kept_rows[q * 32 : (q + 4) * 32, :], lefts)
        for r in range(8):
            kept[r, q : q + 4] = product[:, r * 128 : (r + 1) * 128].reshape(4, 32, 128)


def joined_kernel(core, kept, taken, joined, spun):
    spun[...] = lax.fori_loop(0, core[0] * STAGGER, lambda _, a: a * 0.5 + 0.25, jnp.ones((8, 128), F32))
    for r in range(8):
        joined[r] = (kept[r] + taken[r].astype(F32)).astype(BF16)


def incoming_kernel(core, own, other, operand, products, lefts, arrived):
    pairs = []
    for q in (0, 8):
        for r in range(8):
            lanes = pl.ds(r * 128, 128)
            pairs.append((own.at[r, pl.ds(q, 8)], lefts.at[pl.ds(q, 8), core[0], :, lanes]))
            pairs.append((other.at[r, pl.ds(q, 8)], lefts.at[pl.ds(q, 8), 1 - core[0], :, lanes]))
    pieces = fetch(pairs, arrived)
    rights = jnp.concatenate([operand[r].reshape(512, 128) for r in range(8)], axis=1)
    for b in range(0, 8, 2):
        if b % 4 == 0:
            for piece in pieces[b * 4 : b * 4 + 16]:
                piece.wait()
        product = lax.dot_general(
            rights,
            lefts[b * 2 : b * 2 + 4].reshape(256, 1024),
            (((1,), (1,)), ((), ())),
            preferred_element_type=F32,
        ).astype(BF16)
        for part in range(2):
            products[b + part] = product[:, part * 128 : (part + 1) * 128].reshape(16, 32, 128)


def shape(dims, kind=BF16):
    return jax.ShapeDtypeStruct(dims, kind)


def call(body, outs, scratch, *args, scalars=0, far=0, far_outs=()):
    args = [
        pltpu.with_memory_space_constraint(arg, pltpu.HBM) if scalars <= n < scalars + far else arg
        for n, arg in enumerate(args)
    ]
    vmem, smem, hbm = (pl.BlockSpec(memory_space=space) for space in (pltpu.VMEM, pltpu.SMEM, pltpu.HBM))
    return pl.pallas_call(
        body,
        out_shape=outs,
        in_specs=[smem] * scalars + [hbm] * far + [vmem] * (len(args) - scalars - far),
        out_specs=[hbm if n in far_outs else vmem for n in range(len(outs))],
        scratch_shapes=[
            dims if kind is None else pltpu.VMEM(dims, kind) for dims, kind in scratch
        ],
        compiler_params=pltpu.CompilerParams(vmem_limit_bytes=20 * 1024 * 1024),
    )(*args)


def to_chips(pieces):
    return lax.all_to_all(pieces, CHIPS, split_axis=0, concat_axis=0, tiled=True)


ROWS = ((128 * PITCH, 128), F32)
BLOCKS = ((32, 128, 128), BF16)
WHOLE = ((128, 32, 128), BF16)
SQUARE = ((128, 128), BF16)
GAINS = ((3, 128, 128), F32)
HANDS = ((2, 32 * WIDE, 128), F32)
WEIGHTS = ((512, 128), BF16)
SEND = shape((128, 2, 32, 128))
TURNED = shape(*BLOCKS)
HALF = (8, 16, 32, 128)


def first(pair_rep, proj_weight, in_gain):
    near = [WHOLE, ((4, 128, 128), BF16), ((2, 128), F32)]
    scratch = [*near, ROWS, HANDS, BLOCKS, WEIGHTS, ((128, 128), F32), (pltpu.SemaphoreType.DMA((6,)), None)]
    return call(first_kernel, [SEND, TURNED], scratch, pair_rep, proj_weight, in_gain, far=3)


def side(update_index, *args):
    outs = [shape(BLOCKS[0], F32), shape(*SQUARE), shape(*GAINS), shape(*WEIGHTS)]
    body = functools.partial(side_kernel, update_index)
    return call(body, outs, [BLOCKS, SQUARE], *args)


def copies(number):
    return (pltpu.SemaphoreType.DMA((number,)), None)


def middle(returned, turned, gating, out, gains, weights):
    scratch = [ROWS, HANDS, BLOCKS, BLOCKS, WHOLE, copies(2)]
    outs = [shape(*WHOLE), pltpu.HBM(*WHOLE), TURNED]
    return call(middle_kernel, outs, scratch, returned, turned, gating, out, gains, weights, far_outs=(1,))


def last(returned, turned, gating, out, gains):
    scratch = [ROWS, ROWS, BLOCKS, (BLOCKS[0], F32), WHOLE, copies(4)]
    return call(last_kernel, [shape(*WHOLE)], scratch, returned, turned, gating, out, gains, far_outs=(0,))[0]


def exchanged(pieces):
    return lax.ppermute(pieces, "core", SWAP)


def steps(pair_rep, proj_weight, gate_weight, out_weight, in_gain, out_gain):
    core = lax.axis_index("core").astype(jnp.int32).reshape(1)
    core, pair_rep = lax.optimization_barrier((core, pair_rep))
    parameters = (proj_weight, gate_weight, out_weight, in_gain, out_gain)
    send, turned = first(pair_rep, proj_weight, in_gain)
    operands = to_chips(send).reshape(8, 16, 2, 32, 128)
    gating, out, gains, weights = side(0, turned, *parameters)
    given, kept_rows = call(
        given_kernel,
        [shape(HALF), shape((512, 512))],
        [((512, 1024), BF16), ((1024, 512), BF16)],
        core,
        operands,
        scalars=1,
    )
    taken = exchanged(given)
    (kept,) = call(kept_kernel, [shape(HALF, F32)], [], kept_rows, operands)
    triangle, _ = call(joined_kernel, [shape(HALF), shape((8, 128), F32)], [], core, kept, taken, scalars=1)
    returned = to_chips(triangle.reshape(128, 32, 128))
    left, right, turned = middle(returned, turned, gating, out, gains, weights)
    left = to_chips(left).reshape(HALF)
    right = to_chips(right).reshape(HALF)
    gating, out, gains, _ = side(1, turned, *parameters)
    other = exchanged(left)
    (triangle,) = call(
        incoming_kernel,
        [shape(HALF)],
        [((16, 2, 32, 1024), BF16), copies(32)],
        core,
        left,
        other,
        right,
        scalars=1,
        far=2,
    )
    returned = to_chips(triangle.reshape(128, 32, 128))
    return last(returned, turned, gating, out, gains)


def solution(mesh):
    finer = Mesh(mesh.devices.reshape(8, 16, 2), ("row", "half", "core"))
    placed = (P("row", ("half", "core"), None), P(), P(), P(), P(), P())
    return jax.shard_map(
        steps, mesh=finer, in_specs=placed, out_specs=P("row", ("half", "core"), None), check_vma=False
    )
```

```python
import functools

import jax
import jax.numpy as jnp
from jax import lax
from jax.experimental import pallas as pl
from jax.experimental.pallas import tpu as pltpu
from jax.sharding import Mesh
from jax.sharding import PartitionSpec as P


CHIPS = ("row", "half")
SWAP = [(0, 1), (1, 0)]
F32 = jnp.float32
BF16 = jnp.bfloat16
PITCH = 40
WIDE = 136
STAGGER = 2750


epsilon = 1e-05


def dot(a, b):
    return lax.dot_general(a, b, (((1,), (0,)), ((), ())), preferred_element_type=F32)


def sigmoid(values):
    return 0.5 * jnp.tanh(0.5 * values) + 0.5


def layer_norm(values, gain):
    center = values - jnp.sum(values, axis=0, keepdims=True) * (1.0 / 128)
    spread = jnp.sum(center * center, axis=0, keepdims=True) * (1.0 / 128)
    return center * lax.rsqrt(spread + epsilon) * gain


def column(row):
    return jnp.broadcast_to(row, (128, 128)).T


def turn(matrix):
    return matrix.astype(F32).T.astype(BF16)


def spread_rows(source, scratch, start, groups):
    def step(n, _):
        for part in range(8):
            at = start + n * 8 + part
            scratch[pl.ds(pl.multiple_of(at * PITCH, 8), 32), :] = source[at].astype(F32)
        return _

    lax.fori_loop(0, groups // 8, step, 0)


def each(steps, body):
    def step(j, _):
        body(j)
        return _

    lax.fori_loop(0, steps, step, 0, unroll=8)


def side_by_side(blocks, pair):
    return jnp.concatenate([blocks[pair * 2], blocks[pair * 2 + 1]], axis=1)


def project(normed, weights, hands):
    def body(pair):
        both = side_by_side(normed, pair)
        for side in range(2):
            projected = dot(weights[side * 256 : (side + 1) * 256, :], both)
            hand = sigmoid(projected[0:128]) * projected[128:256]
            for part in range(2):
                at = pl.ds(pl.multiple_of((pair * 2 + part) * WIDE, 8), 128)
                hands[side, at, :] = hand[:, part * 128 : (part + 1) * 128]

    each(16, body)


def gather_side(hands, side, target, start, number):
    def step(n, _):
        for part in range(8):
            h = start + n * 8 + part
            target[h] = hands[side, pl.ds(h, 32, stride=WIDE), :].astype(BF16)
        return _

    lax.fori_loop(0, number // 8, step, 0)


def fetch(pairs, arrived):
    copies = [pltpu.make_async_copy(far, near, arrived.at[n]) for n, (far, near) in enumerate(pairs)]
    for copy in copies:
        copy.start()
    return copies


def first_kernel(x, proj, in_gain, send, turned, x_near, proj_near, gain_near, rows, hands, normed, weights, gains, arrived):
    quarters = [pl.ds(n * 32, 32) for n in range(4)]
    pairs = [(x.at[part], x_near.at[part]) for part in quarters]
    pieces = fetch([(proj.at[0], proj_near), (in_gain, gain_near), *pairs], arrived)
    pieces[0].wait()
    pieces[1].wait()
    for p in range(4):
        weights[p * 128 : (p + 1) * 128, :] = turn(proj_near[p])
    gains[...] = column(gain_near[0:1, :])
    for n in range(4):
        pieces[2 + n].wait()
        spread_rows(x_near, rows, n * 32, 32)

    def body(j):
        channels = rows[pl.ds(j, 128, stride=PITCH), :].T
        turned[j] = channels.astype(BF16)
        normed[j] = layer_norm(channels, gains[...]).astype(BF16)

    each(32, body)
    project(normed, weights, hands)
    for side in range(2):
        gather_side(hands, side, send.at[:, side], 0, 128)


def side_kernel(update_index, turned, proj, gate_w, out_w, in_gain, out_gain, gating, out, gains, weights, normed, gate):
    gate[...], out[...] = turn(gate_w[update_index]), turn(out_w[update_index])
    gains[0] = column(out_gain[update_index : update_index + 1, :])
    gains[1] = column(in_gain[1:2, :])
    gains[2] = column(in_gain[update_index : update_index + 1, :])
    for p in range(4):
        weights[p * 128 : (p + 1) * 128, :] = turn(proj[1, p])

    def norm(j):
        normed[j] = layer_norm(turned[j].astype(F32), gains[2]).astype(BF16)

    each(32, norm)

    def body(pair):
        both = sigmoid(dot(gate[...], side_by_side(normed, pair)))
        for part in range(2):
            gating[pair * 2 + part] = both[:, part * 128 : (part + 1) * 128]

    each(16, body)


def mix(tri, mixed, gains):
    def body(j):
        mixed[j] = layer_norm(tri[pl.ds(j, 128, stride=PITCH), :], gains[0]).astype(BF16)

    each(32, body)


def new_channels(turned, gating, mixed, out, pair):
    change = dot(out[...], side_by_side(mixed, pair))
    return [
        turned[pair * 2 + part].astype(F32) + gating[pair * 2 + part] * change[:, part * 128 : (part + 1) * 128]
        for part in range(2)
    ]


def middle_kernel(returned, turned, gating, out, gains, weights, left, right, newer, tri, hands, mixed, later, right_near, leaving):
    spread_rows(returned, tri, 0, 128)
    mix(tri, mixed, gains)

    def body(pair):
        for part, channels in enumerate(new_channels(turned, gating, mixed, out, pair)):
            rounded = channels.astype(BF16)
            newer[pair * 2 + part] = rounded
            later[pair * 2 + part] = layer_norm(rounded.astype(F32), gains[1]).astype(BF16)

    each(16, body)
    project(later, weights, hands)
    pieces = []
    for n in range(2):
        part = pl.ds(n * 64, 64)
        gather_side(hands, 1, right_near, n * 64, 64)
        pieces.append(pltpu.make_async_copy(right_near.at[part], right.at[part], leaving.at[n]))
        pieces[n].start()
    gather_side(hands, 0, left, 0, 128)
    for piece in pieces:
        piece.wait()


def last_kernel(returned, turned, gating, out, gains, final, tri, rows, mixed, newer, near, left):
    spread_rows(returned, tri, 0, 128)
    mix(tri, mixed, gains)

    def body(pair):
        for part, channels in enumerate(new_channels(turned, gating, mixed, out, pair)):
            newer[pair * 2 + part] = channels

    each(16, body)

    def back(j):
        rows[pl.ds(j, 128, stride=PITCH), :] = newer[j].T

    each(32, back)
    pieces = []
    for n in range(4):

        def collect(m, _):
            for part in range(8):
                at = n * 32 + m * 8 + part
                near[at] = rows[pl.ds(pl.multiple_of(at * PITCH, 8), 32), :].astype(BF16)
            return _

        lax.fori_loop(0, 4, collect, 0)
        pieces.append(pltpu.make_async_copy(near.at[pl.ds(n * 32, 32)], final.at[pl.ds(n * 32, 32)], left.at[n]))
        pieces[n].start()
    for piece in pieces:
        piece.wait()


def side_of(operands, r, side):
    return operands[r, :, side].reshape(512, 128)


def given_kernel(core, operands, given, kept_rows, lefts, turned):
    for r in range(8):
        lefts[:, r * 128 : (r + 1) * 128] = side_of(operands, r, 0)
        turned[r * 128 : (r + 1) * 128, :] = turn(side_of(operands, r, 1))
    for q in range(16):
        kept_rows[q * 32 : (q + 1) * 32, :] = turned[
            pl.ds(pl.multiple_of(q * 64 + core[0] * 32, 32), 32), :
        ]
    for q in range(0, 16, 4):
        block = jnp.concatenate(
            [turned[pl.ds(pl.multiple_of(p * 64 + 32 - core[0] * 32, 32), 32), :] for p in range(q, q + 4)], axis=0
        )
        product = dot(block, lefts[...]).astype(BF16)
        for r in range(8):
            given[r, q : q + 4] = product[:, r * 128 : (r + 1) * 128].reshape(4, 32, 128)


def kept_kernel(kept_rows, operands, kept):
    lefts = jnp.concatenate([side_of(operands, r, 0) for r in range(8)], axis=1)
    for q in range(0, 16, 4):
        product = dot(kept_rows[q * 32 : (q + 4) * 32, :], lefts)
        for r in range(8):
            kept[r, q : q + 4] = product[:, r * 128 : (r + 1) * 128].reshape(4, 32, 128)


def joined_kernel(core, kept, taken, joined, spun):
    spun[...] = lax.fori_loop(0, core[0] * STAGGER, lambda _, a: a * 0.5 + 0.25, jnp.ones((8, 128), F32))
    for r in range(8):
        joined[r] = (kept[r] + taken[r].astype(F32)).astype(BF16)


def lefts_kernel(core, own, other, far_lefts, lefts, arrived, leaving):
    pairs = []
    for r in range(8):
        lanes = pl.ds(r * 128, 128)
        pairs.append((own.at[r], lefts.at[:, core[0], :, lanes]))
        pairs.append((other.at[r], lefts.at[:, 1 - core[0], :, lanes]))
    for piece in fetch(pairs, arrived):
        piece.wait()
    for piece in fetch([(lefts, far_lefts)], leaving):
        piece.wait()


def incoming_kernel(far_lefts, operand, products, lefts, arrived):
    chunks = [pl.ds(q, 4) for q in range(0, 16, 4)]
    pieces = fetch([(far_lefts.at[chunk], lefts.at[chunk]) for chunk in chunks], arrived)
    rights = jnp.concatenate([operand[r].reshape(512, 128) for r in range(8)], axis=1)
    for b in range(0, 8, 2):
        pieces[b // 2].wait()
        product = lax.dot_general(
            rights,
            lefts[b * 2 : b * 2 + 4].reshape(256, 1024),
            (((1,), (1,)), ((), ())),
            preferred_element_type=F32,
        ).astype(BF16)
        for part in range(2):
            products[b + part] = product[:, part * 128 : (part + 1) * 128].reshape(16, 32, 128)


def shape(dims, kind=BF16):
    return jax.ShapeDtypeStruct(dims, kind)


def call(body, outs, scratch, *args, scalars=0, far=0, far_outs=()):
    args = [
        pltpu.with_memory_space_constraint(arg, pltpu.HBM) if scalars <= n < scalars + far else arg
        for n, arg in enumerate(args)
    ]
    vmem, smem, hbm = (pl.BlockSpec(memory_space=space) for space in (pltpu.VMEM, pltpu.SMEM, pltpu.HBM))
    return pl.pallas_call(
        body,
        out_shape=outs,
        in_specs=[smem] * scalars + [hbm] * far + [vmem] * (len(args) - scalars - far),
        out_specs=[hbm if n in far_outs else vmem for n in range(len(outs))],
        scratch_shapes=[
            dims if kind is None else pltpu.VMEM(dims, kind) for dims, kind in scratch
        ],
        compiler_params=pltpu.CompilerParams(vmem_limit_bytes=20 * 1024 * 1024),
    )(*args)


def to_chips(pieces):
    return lax.all_to_all(pieces, CHIPS, split_axis=0, concat_axis=0, tiled=True)


ROWS = ((128 * PITCH, 128), F32)
BLOCKS = ((32, 128, 128), BF16)
WHOLE = ((128, 32, 128), BF16)
SQUARE = ((128, 128), BF16)
GAINS = ((3, 128, 128), F32)
HANDS = ((2, 32 * WIDE, 128), F32)
WEIGHTS = ((512, 128), BF16)
SEND = shape((128, 2, 32, 128))
TURNED = shape(*BLOCKS)
HALF = (8, 16, 32, 128)


def first(pair_rep, proj_weight, in_gain):
    near = [WHOLE, ((4, 128, 128), BF16), ((2, 128), F32)]
    scratch = [*near, ROWS, HANDS, BLOCKS, WEIGHTS, ((128, 128), F32), (pltpu.SemaphoreType.DMA((6,)), None)]
    return call(first_kernel, [SEND, TURNED], scratch, pair_rep, proj_weight, in_gain, far=3)


def side(update_index, *args):
    outs = [shape(BLOCKS[0], F32), shape(*SQUARE), shape(*GAINS), shape(*WEIGHTS)]
    body = functools.partial(side_kernel, update_index)
    return call(body, outs, [BLOCKS, SQUARE], *args)


def copies(number):
    return (pltpu.SemaphoreType.DMA((number,)), None)


def middle(returned, turned, gating, out, gains, weights):
    scratch = [ROWS, HANDS, BLOCKS, BLOCKS, WHOLE, copies(2)]
    outs = [shape(*WHOLE), pltpu.HBM(*WHOLE), TURNED]
    return call(middle_kernel, outs, scratch, returned, turned, gating, out, gains, weights, far_outs=(1,))


def last(returned, turned, gating, out, gains):
    scratch = [ROWS, ROWS, BLOCKS, (BLOCKS[0], F32), WHOLE, copies(4)]
    return call(last_kernel, [shape(*WHOLE)], scratch, returned, turned, gating, out, gains, far_outs=(0,))[0]


def exchanged(pieces):
    return lax.ppermute(pieces, "core", SWAP)


def steps(pair_rep, proj_weight, gate_weight, out_weight, in_gain, out_gain):
    core = lax.axis_index("core").astype(jnp.int32).reshape(1)
    core, pair_rep = lax.optimization_barrier((core, pair_rep))
    parameters = (proj_weight, gate_weight, out_weight, in_gain, out_gain)
    send, turned = first(pair_rep, proj_weight, in_gain)
    operands = to_chips(send).reshape(8, 16, 2, 32, 128)
    gating, out, gains, weights = side(0, turned, *parameters)
    given, kept_rows = call(
        given_kernel,
        [shape(HALF), shape((512, 512))],
        [((512, 1024), BF16), ((1024, 512), BF16)],
        core,
        operands,
        scalars=1,
    )
    taken = exchanged(given)
    (kept,) = call(kept_kernel, [shape(HALF, F32)], [], kept_rows, operands)
    triangle, _ = call(joined_kernel, [shape(HALF), shape((8, 128), F32)], [], core, kept, taken, scalars=1)
    returned = to_chips(triangle.reshape(128, 32, 128))
    left, right, turned = middle(returned, turned, gating, out, gains, weights)
    left = to_chips(left).reshape(HALF)
    right = to_chips(right).reshape(HALF)
    gating, out, gains, _ = side(1, turned, *parameters)
    other = exchanged(left)
    rows = ((16, 2, 32, 1024), BF16)
    (lefts,) = call(
        lefts_kernel, [pltpu.HBM(*rows)], [rows, copies(16), copies(1)], core, left, other, scalars=1, far=2, far_outs=(0,)
    )
    (triangle,) = call(incoming_kernel, [shape(HALF)], [rows, copies(4)], lefts, right, far=1)
    returned = to_chips(triangle.reshape(128, 32, 128))
    return last(returned, turned, gating, out, gains)


def solution(mesh):
    finer = Mesh(mesh.devices.reshape(8, 16, 2), ("row", "half", "core"))
    placed = (P("row", ("half", "core"), None), P(), P(), P(), P(), P())
    return jax.shard_map(
        steps, mesh=finer, in_specs=placed, out_specs=P("row", ("half", "core"), None), check_vma=False
    )
```
